32 devices in a mesh: gx: 4 (over z), gy: 4 (over x, core), gz: 2 (over y).
Axes of the slice: x: 2, y: 2, z: 4, core: 2. Of those that a mesh axis runs over, the one named last changes fastest.
Arguments:
- krylov_basis: float32 [60, 16, 32, 256], P(None, 'gx', 'gy', 'gz'), may hold values from -6 to 6
- schur_vectors: float32 [60, 20], replicated, may hold values from -1 to 1, as said below
- next_vector: float32 [16, 32, 256], P('gx', 'gy', 'gz'), may hold values from -10 to 10
- diag_shift: float32 [16, 32, 256], P('gx', 'gy', 'gz'), may hold values from 0.25 to 2
- velocity: float32 [3, 16, 32, 256], P(None, 'gx', 'gy', 'gz'), may hold values from -1 to 1
Outputs:
- new_basis: float32 [24, 16, 32, 256], P(None, 'gx', 'gy', 'gz')
- hessenberg: float32 [24, 3], replicated
The draws below stay inside these ranges and needn't reach their ends.
Inputs may be any that keep to these rules, and one draw needn't show every extreme that they name: `schur_vectors`: the columns are orthonormal.
All inputs are finite; a program needn't handle non-finite values.
Results may differ from the reference program's by a relative error of at most 0.0003.
Values sent between devices are 32-bit elements; how exact they have to be, the bound alone decides.
A program may use at most 64 MiB of HBM per device.

```python
import jax
import jax.numpy as jnp
from jax import lax

BASIS = 60
KEEP = 20
EXPAND = 3
ROWS = 24
NX = 16
NY = 32
NZ = 256


def draw_schur_vectors(key, part):
    gaussian = jax.random.normal(key, (BASIS, KEEP), jnp.float32)
    orthonormal, triangle = jnp.linalg.qr(gaussian)
    return orthonormal.astype(jnp.float32)


def levels(stream_key, shape, split, least, largest):
    level = 1.0
    for axis_at, parts in split:
        heights = jax.random.uniform(jax.random.fold_in(jax.random.fold_in(stream_key, 6), axis_at), (parts,), jnp.float32, least / len(split), largest / len(split))
        level = level * jnp.repeat(jnp.exp(heights), shape[axis_at] // parts).reshape((-1,) + (1,) * (len(shape) - 1 - axis_at))
    return level


def noise(key, extent, scale, bound, shards=(), dtype=jnp.bfloat16):
    factor_of = levels(key, extent, shards, -0.22, 0.18) if shards else 1.0
    entries = jax.random.normal(key, extent, jnp.float32) * scale * factor_of
    return jnp.minimum(jnp.maximum(entries, -bound), bound).astype(dtype)


def setup_inputs(seed: int = 0) -> dict:
    key_list = jax.random.split(jax.random.key(seed), 6)
    krylov_basis = noise(key_list[0], (BASIS, NX, NY, NZ), 1.0, 6.0, ((1, 4), (2, 4), (3, 2)), jnp.float32)
    schur_vectors = draw_schur_vectors(jax.random.fold_in(key_list[5], 71), 0)
    next_vector = noise(key_list[2], (NX, NY, NZ), 2.0, 10.0, ((0, 4), (1, 4), (2, 2)), jnp.float32)
    diag_shift = jnp.clip(0.25 + 1.75 * jax.random.uniform(key_list[3], (NX, NY, NZ), jnp.float32) ** levels(key_list[3], (NX, NY, NZ), ((0, 4), (1, 4), (2, 2)), -0.2, 0.2), 0.25, 2.0)
    velocity = jnp.clip(jax.random.uniform(key_list[4], (3, NX, NY, NZ), jnp.float32, -1.0, 1.0) * levels(key_list[4], (3, NX, NY, NZ), ((1, 4), (2, 4), (3, 2)), -0.4, 0.0), -1.0, 1.0)
    return {"krylov_basis": krylov_basis, "schur_vectors": schur_vectors, "next_vector": next_vector, "diag_shift": diag_shift, "velocity": velocity}


def operate_field(field, diag_shift, velocity):
    padded = jnp.pad(field, 1)
    x_ahead = padded[2:, 1:-1, 1:-1]
    x_behind = padded[:-2, 1:-1, 1:-1]
    y_ahead = padded[1:-1, 2:, 1:-1]
    y_behind = padded[1:-1, :-2, 1:-1]
    z_ahead = padded[1:-1, 1:-1, 2:]
    z_behind = padded[1:-1, 1:-1, :-2]
    neighbours = x_ahead + x_behind + y_ahead + y_behind + z_ahead + z_behind
    flow = velocity[0] * (x_ahead - x_behind) + velocity[1] * (y_ahead - y_behind) + velocity[2] * (z_ahead - z_behind)
    return (6.0 + diag_shift) * field - neighbours + 0.5 * flow

def reference(krylov_basis, schur_vectors, next_vector, diag_shift, velocity):
    highest = lax.Precision.HIGHEST
    cell_count = NX * NY * NZ
    rotated = jnp.einsum('ik,ixyz->kxyz', schur_vectors, krylov_basis, precision=highest)
    norm_sq = jnp.sum(next_vector * next_vector) / cell_count
    first = next_vector / jnp.maximum(jnp.sqrt(norm_sq), 0.5)
    vectors = jnp.concatenate([rotated, first[None]], axis=0)
    columns = []
    for expansion in range(EXPAND):
        count = vectors.shape[0]
        flat_basis = vectors.reshape(count, -1)
        applied = operate_field(vectors[-1], diag_shift, velocity).reshape(-1)
        first_coeffs = jnp.dot(flat_basis, applied, precision=highest) / cell_count
        partly = applied - jnp.dot(first_coeffs, flat_basis, precision=highest)
        second_coeffs = jnp.dot(flat_basis, partly, precision=highest) / cell_count
        cleaned = partly - jnp.dot(second_coeffs, flat_basis, precision=highest)
        length = jnp.sqrt(jnp.sum(cleaned * cleaned) / cell_count)
        column = jnp.zeros((ROWS,), jnp.float32)
        column = column.at[:count].set(first_coeffs + second_coeffs).at[count].set(length)
        columns.append(column)
        newest = (cleaned / jnp.maximum(length, 0.5)).reshape(NX, NY, NZ)
        vectors = jnp.concatenate([vectors, newest[None]], axis=0)
    return (vectors, jnp.stack(columns, axis=1))
```

```python
import functools

import jax
import jax.numpy as jnp
from jax import lax
from jax.experimental import pallas as pl
from jax.experimental.pallas import tpu as pltpu
from jax.sharding import PartitionSpec as P

KEEP = 20
EXPAND = 3
ROWS = 24
LANES = 128
GROUP = 32
AXES = ("gx", "gy", "gz")


def group_partner(phase, offset, place, sizes):
    ix, iy, iz = place
    nx, ny, nz = sizes
    if phase == 1:
        return (lax.rem(ix + offset, nx), iy, iz)
    other = lax.rem(iy * nz + iz + offset, ny * nz)
    return (ix, other // nz, lax.rem(other, nz))


def body(
    sizes, cells,
    kry_hbm, schur, w_ref, diag, vel,
    out, hess,
    kry, image, xr, yr, zr, ypack, zpack, xh, yh, zh, xs, ys, zs,
    gsend, grecv0, grecv1, rsend, rrecv0, rrecv1,
    load_sem, halo_send, halo_recv, gsem_s0, gsem_r0, gsem_s1, gsem_r1,
    rsem_s0, rsem_r0, rsem_s1, rsem_r1,
):
    place = tuple(lax.axis_index(a) for a in AXES)
    basis = kry.shape[0]
    bx, by, bz = w_ref.shape
    load = pltpu.make_async_copy(kry_hbm, kry, load_sem)
    load.start()
    groups = (sizes[1] * sizes[2], sizes[0])

    for ref in (xr, yr, zr, xs, ys, zs):
        ref[...] = jnp.zeros_like(ref)
    out[KEEP + 1:ROWS] = jnp.zeros((ROWS - KEEP - 1, bx, by, bz), jnp.float32)
    out[KEEP] = w_ref[...]

    barrier = pltpu.get_barrier_semaphore()
    for phase in (0, 1):
        for offset in range(1, groups[phase]):
            pl.semaphore_signal(
                barrier, inc=1,
                device_id=group_partner(phase, offset, place, sizes),
                device_id_type=pl.DeviceIdType.MESH,
            )
    pl.semaphore_wait(barrier, groups[0] + groups[1] - 2)

    def halo_copies(kind, sources, targets):
        found = []
        for d in range(3):
            for side in (0, 1):
                at = (kind * 3 + d) * 2 + side
                to = list(place)
                to[d] = place[d] + (1 if side == 0 else -1)
                can_send = place[d] < sizes[d] - 1 if side == 0 else place[d] > 0
                can_recv = place[d] > 0 if side == 0 else place[d] < sizes[d] - 1
                found.append((
                    pltpu.make_async_remote_copy(
                        src_ref=sources[d][side], dst_ref=targets[d][side],
                        send_sem=halo_send.at[at], recv_sem=halo_recv.at[at],
                        device_id=tuple(to), device_id_type=pl.DeviceIdType.MESH,
                    ), can_send, can_recv))
        return found

    def halo_start(copies):
        for copy, can_send, _ in copies:
            pl.when(can_send)(copy.start)

    def halo_wait(copies):
        for copy, _, can_recv in copies:
            pl.when(can_recv)(copy.wait_recv)

    def halo_finish(copies):
        for copy, can_send, _ in copies:
            pl.when(can_send)(copy.wait_send)

    def field_copies(kind, ref):
        return halo_copies(
            kind,
            ((ref.at[bx - 1], ref.at[0]), (ref, ref), (ref, ref)),
            tuple((r.at[kind, 0], r.at[kind, 1]) for r in (xs, ys, zs)),
        )

    def exchange(send, slots, sems_s, sems_r, phase):
        copies = []
        for offset in range(1, groups[phase]):
            copies.append(pltpu.make_async_remote_copy(
                src_ref=send, dst_ref=slots.at[offset - 1],
                send_sem=sems_s.at[offset - 1], recv_sem=sems_r.at[offset - 1],
                device_id=group_partner(phase, offset, place, sizes),
                device_id_type=pl.DeviceIdType.MESH,
            ))
        for copy in copies:
            copy.start()
        return copies

    def gather_sum(copies, own, slots):
        for copy in copies:
            copy.wait_recv()
        for k in range(len(copies)):
            own = own + slots[k]
        return own

    lane3 = lax.broadcasted_iota(jnp.int32, (by, bz), 1)
    row3 = lax.broadcasted_iota(jnp.int32, (by, bz), 0)

    def stencil(v, x_before, x_after, y_before, y_after, z_before, z_after):
        res = []
        for x in range(bx):
            here = v[x]
            xb = v[x - 1] if x > 0 else x_before
            xa = v[x + 1] if x < bx - 1 else x_after
            yb = jnp.where(row3 == 0, y_before[x], pltpu.roll(here, 1, 0))
            ya = jnp.where(row3 == by - 1, y_after[x], pltpu.roll(here, by - 1, 0))
            zb = jnp.where(lane3 == 0, z_before[x], pltpu.roll(here, 1, 1))
            za = jnp.where(lane3 == bz - 1, z_after[x], pltpu.roll(here, bz - 1, 1))
            neighbours = xa + xb + ya + yb + za + zb
            flow = (vel[0, x] * (xa - xb) + vel[1, x] * (ya - yb) + vel[2, x] * (za - zb))
            res.append((6.0 + diag[x]) * here - neighbours + 0.5 * flow)
        return res

    def dots(v, count):
        parts = []
        for i in range(ROWS):
            if i < count:
                total = out[i, 0] * v[0]
                for x in range(1, bx):
                    total = total + out[i, x] * v[x]
            elif i == ROWS - 1:
                total = v[0] * v[0]
                for x in range(1, bx):
                    total = total + v[x] * v[x]
            else:
                total = None
            parts.append(jnp.zeros((1, bz), jnp.float32) if total is None
                         else jnp.sum(total, axis=0, keepdims=True))
        return jnp.sum(jnp.concatenate(parts, axis=0), axis=1, keepdims=True)

    halo_w = field_copies(0, w_ref)
    halo_start(halo_w)

    load.wait()
    wide, deep = 5, 4
    for first in range(0, KEEP, wide):
        def step(at, sums, first=first):
            sums = list(sums)
            for k in range(deep):
                i = at * deep + k
                for x in range(bx):
                    tile = kry[i, x]
                    for j in range(wide):
                        sums[j * bx + x] = sums[j * bx + x] + schur[i, first + j] * tile
            return tuple(sums)
        sums = lax.fori_loop(
            0, basis // deep, step,
            tuple(jnp.zeros((by, bz), jnp.float32) for _ in range(wide * bx)))
        for j in range(wide):
            for x in range(bx):
                out[first + j, x] = sums[j * bx + x]

    for side, (row, edge) in enumerate(((by - 1, bz - 1), (0, 0))):
        for i in range(KEEP):
            ypack[side, i] = out[i, :, row, :]
        for x in range(bx):
            packed = jnp.zeros((by, bz), jnp.float32)
            for i in range(KEEP):
                packed = jnp.where(
                    lane3 == i, pltpu.roll(out[i, x], (i - edge) % bz, 1), packed)
            zpack[side, x] = packed
    halo_r = halo_copies(
        3,
        ((out.at[0:KEEP, bx - 1], out.at[0:KEEP, 0]), (ypack.at[0], ypack.at[1]),
         (zpack.at[0], zpack.at[1])),
        tuple((r.at[0], r.at[1]) for r in (xr, yr, zr)),
    )
    halo_start(halo_r)

    row = lax.broadcasted_iota(jnp.int32, (ROWS, LANES), 0)
    lane = lax.broadcasted_iota(jnp.int32, (ROWS, LANES), 1)
    lane1 = lax.broadcasted_iota(jnp.int32, (1, LANES), 1)
    row1 = lax.broadcasted_iota(jnp.int32, (ROWS, 1), 0)

    gram = jnp.zeros((ROWS, LANES), jnp.float32)
    for j in range(KEEP + 1):
        col = dots([out[j, x] for x in range(bx)], KEEP + 1)
        gram = jnp.where(lane == j, jnp.where(row < KEEP + 1, col, 0.0), gram)

    halo_wait(halo_w)
    applied = stencil(
        [w_ref[x] for x in range(bx)], xs[0, 0], xs[0, 1],
        [ys[0, 0, x, by - 1:by, :] for x in range(bx)],
        [ys[0, 1, x, 0:1, :] for x in range(bx)],
        [zs[0, 0, x, :, bz - 1:bz] for x in range(bx)],
        [zs[0, 1, x, :, 0:1] for x in range(bx)],
    )
    for x in range(bx):
        image[0, x] = applied[x]
    halo_a = field_copies(1, image.at[0])
    halo_start(halo_a)
    col = dots(applied, KEEP + 1)
    gram = jnp.where(lane == ROWS - 1, col, gram)
    packed = jnp.zeros((8, LANES), jnp.float32)
    for part in range(ROWS // 8):
        piece = gram[part * 8:part * 8 + 8]
        packed = packed + (pltpu.roll(piece, part * GROUP, 1) if part else piece)
    gsend[0] = packed
    copies0 = exchange(gsend.at[0], grecv0, gsem_s0, gsem_r0, 0)
    packed = gather_sum(copies0, packed, grecv0)
    gsend[1] = packed
    copies1 = exchange(gsend.at[1], grecv1, gsem_s1, gsem_r1, 1)
    packed = gather_sum(copies1, packed, grecv1) * (1.0 / cells)
    pending = [copies0, copies1]
    gram = jnp.concatenate(
        [packed] + [pltpu.roll(packed, LANES - part * GROUP, 1) for part in range(1, ROWS // 8)],
        axis=0)

    c_col = jnp.sum(jnp.where(lane == ROWS - 1, gram, 0.0), axis=1, keepdims=True)
    gram = jnp.where((lane < KEEP + 1) & (row < KEEP + 1), gram, 0.0)
    norm_sq = jnp.sum(
        jnp.sum(jnp.where((lane == KEEP) & (row == KEEP), gram, 0.0), axis=1, keepdims=True),
        axis=0, keepdims=True)
    scale = 1.0 / jnp.maximum(jnp.sqrt(norm_sq), 0.5)
    gram = gram * jnp.where(row == KEEP, scale, 1.0) * jnp.where(lane == KEEP, scale, 1.0)
    c_col = c_col * scale * jnp.where((row1 == KEEP) | (row1 == ROWS - 1), scale, 1.0)
    for x in range(bx):
        out[KEEP, x] = w_ref[x] * scale
    applied = [tile * scale for tile in applied]

    halo_wait(halo_r)
    for side in (0, 1):
        near_row, near_lane = (by - 1, bz - 1) if side == 0 else (0, 0)
        xh[side, 0] = xs[0, side] * scale
        for x in range(bx):
            yh[side, 0, x:x + 1] = ys[0, side, x, near_row:near_row + 1, :] * scale
            zh[side, x] = jnp.where(
                lane3 == KEEP, zs[0, side, x, :, near_lane:near_lane + 1] * scale, zr[side, x])
    halos = {1: halo_a}
    hcols = []
    for k in range(EXPAND):
        count = KEEP + 1 + k
        if k > 0:
            rowform = jnp.sum(jnp.where(row == lane, dots(applied, count), 0.0),
                              axis=0, keepdims=True)
            rsend[k - 1, 0] = rowform
            copies0 = exchange(rsend.at[k - 1, 0], rrecv0.at[k - 1],
                               rsem_s0.at[k - 1], rsem_r0.at[k - 1], 0)
            rowform = gather_sum(copies0, rowform, rrecv0.at[k - 1])
            rsend[k - 1, 1] = rowform
            copies1 = exchange(rsend.at[k - 1, 1], rrecv1.at[k - 1],
                               rsem_s1.at[k - 1], rsem_r1.at[k - 1], 1)
            rowform = gather_sum(copies1, rowform, rrecv1.at[k - 1]) * (1.0 / cells)
            pending += [copies0, copies1]
            c_col = jnp.sum(jnp.where(row == lane, rowform, 0.0), axis=1, keepdims=True)
        else:
            rowform = jnp.sum(jnp.where(row == lane, c_col, 0.0), axis=0, keepdims=True)
        self_norm = jnp.sum(jnp.where(lane1 == ROWS - 1, rowform, 0.0), axis=1, keepdims=True)
        c_col = jnp.where(row1 < count, c_col, 0.0)
        c_row = jnp.where(lane1 < count, rowform, 0.0)
        e_col = c_col - jnp.sum(gram * c_row, axis=1, keepdims=True)
        e_row = c_row - jnp.sum(gram * c_col, axis=0, keepdims=True)
        t_col, t_row = c_col + e_col, c_row + e_row
        gt_row = jnp.sum(gram * t_col, axis=0, keepdims=True)
        length_sq = self_norm + jnp.sum(t_row * (gt_row - 2.0 * c_row), axis=1, keepdims=True)
        length_sq = jnp.maximum(length_sq, 0.0)
        length = jnp.sqrt(length_sq)
        inverse = 1.0 / jnp.maximum(length, 0.5)
        hcols.append(jnp.where(row1 == count, length, t_col))
        weights = jnp.broadcast_to(t_col * inverse, (ROWS, LANES))
        newest = [tile * inverse for tile in applied]
        for i in range(count):
            weight = jnp.broadcast_to(weights[i:i + 1, :], (by, bz))
            for x in range(bx):
                newest[x] = newest[x] - weight * out[i, x]
        for x in range(bx):
            out[count, x] = newest[x]
        if k == EXPAND - 1:
            break
        halo_wait(halos[k + 1])
        sides = []
        for side in (0, 1):
            near_row, near_lane = (by - 1, bz - 1) if side == 0 else (0, 0)
            factor = scale * inverse if k == 0 else inverse
            x_part = xs[k + 1, side] * factor
            y_part = [ys[k + 1, side, x, near_row:near_row + 1, :] * factor for x in range(bx)]
            y_part = jnp.concatenate(y_part, axis=0)
            for i in range(count):
                weight = weights[i:i + 1, :]
                if i < KEEP:
                    x_part = x_part - weight * xr[side, i]
                    y_part = y_part - weight * yr[side, i]
                else:
                    x_part = x_part - weight * xh[side, i - KEEP]
                    y_part = y_part - weight * yh[side, i - KEEP]
            z_part = []
            for x in range(bx):
                column = (zs[k + 1, side, x, :, near_lane:near_lane + 1] * factor
                          - jnp.sum(zh[side, x] * (t_row * inverse), axis=1, keepdims=True))
                z_part.append(column)
                if k + 1 < EXPAND - 1:
                    zh[side, x] = jnp.where(lane3 == count, column, zh[side, x])
            xh[side, count - KEEP] = x_part
            yh[side, count - KEEP] = y_part
            sides.append((x_part, [y_part[x:x + 1] for x in range(bx)], z_part))
        applied = stencil(newest, sides[0][0], sides[1][0], sides[0][1], sides[1][1],
                          sides[0][2], sides[1][2])
        if k + 1 < EXPAND - 1:
            for x in range(bx):
                image[1, x] = applied[x]
            halos[k + 2] = field_copies(k + 2, image.at[1])
            halo_start(halos[k + 2])
        cross_col = (e_col - jnp.sum(gram * e_row, axis=1, keepdims=True)) * inverse
        cross_row = (e_row - jnp.sum(gram * e_col, axis=0, keepdims=True)) * inverse
        corner = length_sq * inverse * inverse
        gram = jnp.where(row == count, cross_row, jnp.where(lane == count, cross_col, gram))
        gram = jnp.where((row == count) & (lane == count), corner, gram)

    hess[...] = jnp.concatenate(hcols, axis=1)
    halo_finish(halo_w)
    halo_finish(halo_r)
    for copies in halos.values():
        halo_finish(copies)
    for copies in pending:
        for copy in copies:
            copy.wait_send()


def per_device(krylov_basis, schur_vectors, next_vector, diag_shift, velocity):
    sizes = tuple(lax.axis_size(a) for a in AXES)
    block = next_vector.shape
    bx, by, bz = block
    cells = float(bx * by * bz * sizes[0] * sizes[1] * sizes[2])
    n0, n1 = sizes[1] * sizes[2], sizes[0]
    small = EXPAND - 1
    f32 = jnp.float32
    vmem = pl.BlockSpec(memory_space=pltpu.VMEM)
    dma = pltpu.SemaphoreType.DMA
    return pl.pallas_call(
        functools.partial(body, sizes, cells),
        out_shape=(
            jax.ShapeDtypeStruct((ROWS,) + block, f32),
            jax.ShapeDtypeStruct((ROWS, EXPAND), f32),
        ),
        in_specs=[
            pl.BlockSpec(memory_space=pl.ANY),
            pl.BlockSpec(memory_space=pltpu.SMEM),
            vmem, vmem, vmem,
        ],
        out_specs=(vmem, vmem),
        scratch_shapes=[
            pltpu.VMEM(krylov_basis.shape, f32),
            pltpu.VMEM((2,) + block, f32),
            pltpu.VMEM((2, KEEP, by, bz), f32),
            pltpu.VMEM((2, KEEP, bx, bz), f32),
            pltpu.VMEM((2,) + block, f32),
            pltpu.VMEM((2, KEEP, bx, bz), f32),
            pltpu.VMEM((2,) + block, f32),
            pltpu.VMEM((2, EXPAND, by, bz), f32),
            pltpu.VMEM((2, EXPAND, bx, bz), f32),
            pltpu.VMEM((2,) + block, f32),
            pltpu.VMEM((EXPAND, 2, by, bz), f32),
            pltpu.VMEM((EXPAND, 2) + block, f32),
            pltpu.VMEM((EXPAND, 2) + block, f32),
            pltpu.VMEM((2, 8, LANES), f32),
            pltpu.VMEM((n0 - 1, 8, LANES), f32),
            pltpu.VMEM((n1 - 1, 8, LANES), f32),
            pltpu.VMEM((small, 2, 1, LANES), f32),
            pltpu.VMEM((small, n0 - 1, 1, LANES), f32),
            pltpu.VMEM((small, n1 - 1, 1, LANES), f32),
            dma, dma((24,)), dma((24,)),
            dma((n0 - 1,)), dma((n0 - 1,)), dma((n1 - 1,)), dma((n1 - 1,)),
            dma((small, n0 - 1)), dma((small, n0 - 1)),
            dma((small, n1 - 1)), dma((small, n1 - 1)),
        ],
        compiler_params=pltpu.CompilerParams(collective_id=0, has_side_effects=True),
    )(krylov_basis, schur_vectors, next_vector, diag_shift, velocity)


def solution(mesh):
    in_specs = (
        P(None, "gx", "gy", "gz"),
        P(),
        P("gx", "gy", "gz"),
        P("gx", "gy", "gz"),
        P(None, "gx", "gy", "gz"),
    )
    out_specs = (P(None, "gx", "gy", "gz"), P())
    return jax.shard_map(
        per_device, mesh=mesh, in_specs=in_specs, out_specs=out_specs, check_vma=False
    )
```

```python
import functools

import jax
import jax.numpy as jnp
from jax import lax
from jax.experimental import pallas as pl
from jax.experimental.pallas import tpu as pltpu
from jax.sharding import PartitionSpec as P

KEEP = 20
EXPAND = 3
ROWS = 24
LANES = 128
GROUP = 32
DIRECT = 64
AXES = ("gx", "gy", "gz")


def group_partner(phase, offset, place, sizes):
    ix, iy, iz = place
    nx, ny, nz = sizes
    if phase == 1:
        return (lax.rem(ix + offset, nx), iy, iz)
    if phase == 2:
        other = lax.rem((ix * ny + iy) * nz + iz + offset, nx * ny * nz)
        return (other // (ny * nz), lax.rem(other // nz, ny), lax.rem(other, nz))
    other = lax.rem(iy * nz + iz + offset, ny * nz)
    return (ix, other // nz, lax.rem(other, nz))


def body(
    sizes, cells,
    kry_hbm, schur, w_ref, diag, vel,
    out, hess,
    kry, image, xr, yr, zr, ypack, zpack, xh, yh, zh, xs, ys, zs,
    gsend, grecv0, grecv1, rsend, rrecv0, rrecv1, mid,
    load_sem, halo_send, halo_recv, gsem_s0, gsem_r0, gsem_s1, gsem_r1,
    rsem_s0, rsem_r0, rsem_s1, rsem_r1, ready,
):
    place = tuple(lax.axis_index(a) for a in AXES)
    basis = kry.shape[0]
    bx, by, bz = w_ref.shape
    load = pltpu.make_async_copy(kry_hbm, kry, load_sem)
    load.start()
    groups = (sizes[1] * sizes[2], sizes[0], sizes[0] * sizes[1] * sizes[2])
    direct = groups[2] <= DIRECT

    for ref in (xr, yr, zr, xs, ys, zs):
        ref[...] = jnp.zeros_like(ref)
    out[KEEP + 1:ROWS] = jnp.zeros((ROWS - KEEP - 1, bx, by, bz), jnp.float32)
    out[KEEP] = w_ref[...]

    barrier = pltpu.get_barrier_semaphore()
    for phase in (0, 1):
        for offset in range(1, groups[phase]):
            pl.semaphore_signal(
                barrier, inc=1,
                device_id=group_partner(phase, offset, place, sizes),
                device_id_type=pl.DeviceIdType.MESH,
            )
    pl.semaphore_wait(barrier, groups[0] + groups[1] - 2)

    def halo_copies(kind, sources, targets):
        found = []
        for d in range(3):
            for side in (0, 1):
                at = (kind * 3 + d) * 2 + side
                to = list(place)
                to[d] = place[d] + (1 if side == 0 else -1)
                can_send = place[d] < sizes[d] - 1 if side == 0 else place[d] > 0
                can_recv = place[d] > 0 if side == 0 else place[d] < sizes[d] - 1
                found.append((
                    pltpu.make_async_remote_copy(
                        src_ref=sources[d][side], dst_ref=targets[d][side],
                        send_sem=halo_send.at[at], recv_sem=halo_recv.at[at],
                        device_id=tuple(to), device_id_type=pl.DeviceIdType.MESH,
                    ), can_send, can_recv))
        return found

    def halo_start(copies):
        for copy, can_send, _ in copies:
            pl.when(can_send)(copy.start)

    def halo_wait(copies):
        for copy, _, can_recv in copies:
            pl.when(can_recv)(copy.wait_recv)

    def halo_finish(copies):
        for copy, can_send, _ in copies:
            pl.when(can_send)(copy.wait_send)

    def field_copies(kind, ref):
        return halo_copies(
            kind,
            ((ref.at[bx - 1], ref.at[0]), (ref, ref), (ref, ref)),
            tuple((r.at[kind, 0], r.at[kind, 1]) for r in (xs, ys, zs)),
        )

    def exchange(send, slots, sems_s, sems_r, phase):
        copies = []
        for offset in range(1, groups[phase]):
            copies.append(pltpu.make_async_remote_copy(
                src_ref=send, dst_ref=slots.at[offset - 1],
                send_sem=sems_s.at[offset - 1], recv_sem=sems_r.at[offset - 1],
                device_id=group_partner(phase, offset, place, sizes),
                device_id_type=pl.DeviceIdType.MESH,
            ))
        for copy in copies:
            copy.start()
        return copies

    def gather_sum(copies, own, slots):
        for copy in copies:
            copy.wait_recv()
        terms = [own] + [slots[k] for k in range(len(copies))]
        while len(terms) > 1:
            terms = [sum(terms[k:k + 2]) for k in range(0, len(terms), 2)]
        return terms[0]

    pending = []

    def row_start(k, rowform):
        rsend[k] = rowform
        phase = 2 if direct else 0
        copies = exchange(rsend.at[k], rrecv0.at[k], rsem_s0.at[k], rsem_r0.at[k], phase)
        pending.append(copies)
        return copies

    def row_end(k, rowform, copies):
        rowform = gather_sum(copies, rowform, rrecv0.at[k])
        if not direct:
            mid[k] = rowform
            copies = exchange(mid.at[k], rrecv1.at[k], rsem_s1.at[k], rsem_r1.at[k], 1)
            pending.append(copies)
            rowform = gather_sum(copies, rowform, rrecv1.at[k])
        return rowform * (1.0 / cells)

    lane3 = lax.broadcasted_iota(jnp.int32, (by, bz), 1)
    row3 = lax.broadcasted_iota(jnp.int32, (by, bz), 0)

    def stencil(v, x_before, x_after, y_before, y_after, z_before, z_after):
        res = []
        for x in range(bx):
            here = v[x]
            xb = v[x - 1] if x > 0 else x_before
            xa = v[x + 1] if x < bx - 1 else x_after
            yb = jnp.where(row3 == 0, y_before[x], pltpu.roll(here, 1, 0))
            ya = jnp.where(row3 == by - 1, y_after[x], pltpu.roll(here, by - 1, 0))
            zb = jnp.where(lane3 == 0, z_before[x], pltpu.roll(here, 1, 1))
            za = jnp.where(lane3 == bz - 1, z_after[x], pltpu.roll(here, bz - 1, 1))
            neighbours = xa + xb + ya + yb + za + zb
            flow = (vel[0, x] * (xa - xb) + vel[1, x] * (ya - yb) + vel[2, x] * (za - zb))
            res.append((6.0 + diag[x]) * here - neighbours + 0.5 * flow)
        return res

    def dots(v, count):
        parts = []
        for i in range(ROWS):
            if i < count:
                total = out[i, 0] * v[0]
                for x in range(1, bx):
                    total = total + out[i, x] * v[x]
            elif i == ROWS - 1:
                total = v[0] * v[0]
                for x in range(1, bx):
                    total = total + v[x] * v[x]
            else:
                total = None
            parts.append(jnp.zeros((1, bz), jnp.float32) if total is None
                         else jnp.sum(total, axis=0, keepdims=True))
        return jnp.sum(jnp.concatenate(parts, axis=0), axis=1, keepdims=True)

    halo_w = field_copies(0, w_ref)
    halo_start(halo_w)
    if direct:
        for offset in range(1, groups[1]):
            pl.semaphore_signal(
                ready, inc=1, device_id=group_partner(1, offset, place, sizes),
                device_id_type=pl.DeviceIdType.MESH)

    load.wait()
    wide, deep = 5, 4
    for first in range(0, KEEP, wide):
        def step(at, sums, first=first):
            sums = list(sums)
            for k in range(deep):
                i = at * deep + k
                for x in range(bx):
                    tile = kry[i, x]
                    for j in range(wide):
                        sums[j * bx + x] = sums[j * bx + x] + schur[first + j, i] * tile
            return tuple(sums)
        sums = lax.fori_loop(
            0, basis // deep, step,
            tuple(jnp.zeros((by, bz), jnp.float32) for _ in range(wide * bx)))
        for j in range(wide):
            for x in range(bx):
                out[first + j, x] = sums[j * bx + x]

    for side, (row, edge) in enumerate(((by - 1, bz - 1), (0, 0))):
        for i in range(KEEP):
            ypack[side, i] = out[i, :, row, :]
        for x in range(bx):
            packed = jnp.zeros((by, bz), jnp.float32)
            for i in range(KEEP):
                packed = jnp.where(
                    lane3 == i, pltpu.roll(out[i, x], (i - edge) % bz, 1), packed)
            zpack[side, x] = packed
    halo_r = halo_copies(
        3,
        ((out.at[0:KEEP, bx - 1], out.at[0:KEEP, 0]), (ypack.at[0], ypack.at[1]),
         (zpack.at[0], zpack.at[1])),
        tuple((r.at[0], r.at[1]) for r in (xr, yr, zr)),
    )
    halo_start(halo_r)

    row = lax.broadcasted_iota(jnp.int32, (ROWS, LANES), 0)
    lane = lax.broadcasted_iota(jnp.int32, (ROWS, LANES), 1)
    lane1 = lax.broadcasted_iota(jnp.int32, (1, LANES), 1)
    row1 = lax.broadcasted_iota(jnp.int32, (ROWS, 1), 0)

    gram = jnp.zeros((ROWS, LANES), jnp.float32)
    for j in range(KEEP + 1):
        col = dots([out[j, x] for x in range(bx)], KEEP + 1)
        gram = jnp.where(lane == j, jnp.where(row < KEEP + 1, col, 0.0), gram)

    packed = jnp.zeros((8, LANES), jnp.float32)
    for part in range(ROWS // 8):
        piece = gram[part * 8:part * 8 + 8]
        packed = packed + (pltpu.roll(piece, part * GROUP, 1) if part else piece)
    gsend[0] = packed
    gcopies0 = exchange(gsend.at[0], grecv0, gsem_s0, gsem_r0, 0)

    halo_wait(halo_w)
    applied = stencil(
        [w_ref[x] for x in range(bx)], xs[0, 0], xs[0, 1],
        [ys[0, 0, x, by - 1:by, :] for x in range(bx)],
        [ys[0, 1, x, 0:1, :] for x in range(bx)],
        [zs[0, 0, x, :, bz - 1:bz] for x in range(bx)],
        [zs[0, 1, x, :, 0:1] for x in range(bx)],
    )
    for x in range(bx):
        image[0, x] = applied[x]
    ownrow = jnp.sum(jnp.where(row == lane, dots(applied, KEEP + 1), 0.0),
                     axis=0, keepdims=True)
    if direct:
        pl.semaphore_wait(ready, groups[1] - 1)
    copies = row_start(0, ownrow)
    halo_a = field_copies(1, image.at[0])
    halo_start(halo_a)

    packed = gather_sum(gcopies0, packed, grecv0)
    gsend[1] = packed
    gcopies1 = exchange(gsend.at[1], grecv1, gsem_s1, gsem_r1, 1)
    packed = gather_sum(gcopies1, packed, grecv1) * (1.0 / cells)
    pending += [gcopies0, gcopies1]
    gram = jnp.concatenate(
        [packed] + [pltpu.roll(packed, LANES - part * GROUP, 1) for part in range(1, ROWS // 8)],
        axis=0)
    gram = jnp.where((lane < KEEP + 1) & (row < KEEP + 1), gram, 0.0)
    norm_sq = jnp.sum(
        jnp.sum(jnp.where((lane == KEEP) & (row == KEEP), gram, 0.0), axis=1, keepdims=True),
        axis=0, keepdims=True)
    scale = 1.0 / jnp.maximum(jnp.sqrt(norm_sq), 0.5)
    gram = gram * jnp.where(row == KEEP, scale, 1.0) * jnp.where(lane == KEEP, scale, 1.0)
    for x in range(bx):
        out[KEEP, x] = w_ref[x] * scale
    applied = [tile * scale for tile in applied]
    rowform = row_end(0, ownrow, copies)
    rowform = rowform * scale * jnp.where((lane1 == KEEP) | (lane1 == ROWS - 1), scale, 1.0)

    halo_wait(halo_r)
    for side in (0, 1):
        near_row, near_lane = (by - 1, bz - 1) if side == 0 else (0, 0)
        xh[side, 0] = xs[0, side] * scale
        for x in range(bx):
            yh[side, 0, x:x + 1] = ys[0, side, x, near_row:near_row + 1, :] * scale
            zh[side, x] = jnp.where(
                lane3 == KEEP, zs[0, side, x, :, near_lane:near_lane + 1] * scale, zr[side, x])
    halos = {1: halo_a}
    hcols = []
    for k in range(EXPAND):
        count = KEEP + 1 + k
        if k > 0:
            rowform = jnp.sum(jnp.where(row == lane, dots(applied, count), 0.0),
                              axis=0, keepdims=True)
            rowform = row_end(k, rowform, row_start(k, rowform))
        c_col = jnp.sum(jnp.where(row == lane, rowform, 0.0), axis=1, keepdims=True)
        self_norm = jnp.sum(jnp.where(lane1 == ROWS - 1, rowform, 0.0), axis=1, keepdims=True)
        c_col = jnp.where(row1 < count, c_col, 0.0)
        c_row = jnp.where(lane1 < count, rowform, 0.0)
        e_col = c_col - jnp.sum(gram * c_row, axis=1, keepdims=True)
        e_row = c_row - jnp.sum(gram * c_col, axis=0, keepdims=True)
        t_col, t_row = c_col + e_col, c_row + e_row
        gt_row = jnp.sum(gram * t_col, axis=0, keepdims=True)
        length_sq = self_norm + jnp.sum(t_row * (gt_row - 2.0 * c_row), axis=1, keepdims=True)
        length_sq = jnp.maximum(length_sq, 0.0)
        length = jnp.sqrt(length_sq)
        inverse = 1.0 / jnp.maximum(length, 0.5)
        hcols.append(jnp.where(row1 == count, length, t_col))
        weights = jnp.broadcast_to(t_col * inverse, (ROWS, LANES))
        newest = [tile * inverse for tile in applied]
        for i in range(count):
            weight = jnp.broadcast_to(weights[i:i + 1, :], (by, bz))
            for x in range(bx):
                newest[x] = newest[x] - weight * out[i, x]
        for x in range(bx):
            out[count, x] = newest[x]
        if k == EXPAND - 1:
            break
        halo_wait(halos[k + 1])
        sides = []
        for side in (0, 1):
            near_row, near_lane = (by - 1, bz - 1) if side == 0 else (0, 0)
            factor = scale * inverse if k == 0 else inverse
            x_part = xs[k + 1, side] * factor
            y_part = [ys[k + 1, side, x, near_row:near_row + 1, :] * factor for x in range(bx)]
            y_part = jnp.concatenate(y_part, axis=0)
            for i in range(count):
                weight = weights[i:i + 1, :]
                if i < KEEP:
                    x_part = x_part - weight * xr[side, i]
                    y_part = y_part - weight * yr[side, i]
                else:
                    x_part = x_part - weight * xh[side, i - KEEP]
                    y_part = y_part - weight * yh[side, i - KEEP]
            z_part = []
            for x in range(bx):
                column = (zs[k + 1, side, x, :, near_lane:near_lane + 1] * factor
                          - jnp.sum(zh[side, x] * (t_row * inverse), axis=1, keepdims=True))
                z_part.append(column)
                if k + 1 < EXPAND - 1:
                    zh[side, x] = jnp.where(lane3 == count, column, zh[side, x])
            xh[side, count - KEEP] = x_part
            yh[side, count - KEEP] = y_part
            sides.append((x_part, [y_part[x:x + 1] for x in range(bx)], z_part))
        applied = stencil(newest, sides[0][0], sides[1][0], sides[0][1], sides[1][1],
                          sides[0][2], sides[1][2])
        if k + 1 < EXPAND - 1:
            for x in range(bx):
                image[1, x] = applied[x]
            halos[k + 2] = field_copies(k + 2, image.at[1])
            halo_start(halos[k + 2])
        cross_col = (e_col - jnp.sum(gram * e_row, axis=1, keepdims=True)) * inverse
        cross_row = (e_row - jnp.sum(gram * e_col, axis=0, keepdims=True)) * inverse
        corner = length_sq * inverse * inverse
        gram = jnp.where(row == count, cross_row, jnp.where(lane == count, cross_col, gram))
        gram = jnp.where((row == count) & (lane == count), corner, gram)

    for k in range(EXPAND):
        hess[k:k + 1] = jnp.sum(
            jnp.where(row == lane, hcols[k % len(hcols)], 0.0), axis=0, keepdims=True)
    halo_finish(halo_w)
    halo_finish(halo_r)
    for copies in halos.values():
        halo_finish(copies)
    for copies in pending:
        for copy in copies:
            copy.wait_send()


def per_device(krylov_basis, schur_vectors, next_vector, diag_shift, velocity):
    sizes = tuple(lax.axis_size(a) for a in AXES)
    block = next_vector.shape
    bx, by, bz = block
    cells = float(bx * by * bz * sizes[0] * sizes[1] * sizes[2])
    n0, n1 = sizes[1] * sizes[2], sizes[0]
    nrow = n0 * n1 if n0 * n1 <= DIRECT else n0
    f32 = jnp.float32
    vmem = pl.BlockSpec(memory_space=pltpu.VMEM)
    dma = pltpu.SemaphoreType.DMA
    vectors, columns = pl.pallas_call(
        functools.partial(body, sizes, cells),
        out_shape=(
            pltpu.VMEM((ROWS,) + block, f32),
            pltpu.VMEM((8, LANES), f32),
        ),
        in_specs=[
            pl.BlockSpec(memory_space=pl.ANY),
            pl.BlockSpec(memory_space=pltpu.SMEM),
            vmem, vmem, vmem,
        ],
        out_specs=(vmem, vmem),
        scratch_shapes=[
            pltpu.VMEM(krylov_basis.shape, f32),
            pltpu.VMEM((2,) + block, f32),
            pltpu.VMEM((2, KEEP, by, bz), f32),
            pltpu.VMEM((2, KEEP, bx, bz), f32),
            pltpu.VMEM((2,) + block, f32),
            pltpu.VMEM((2, KEEP, bx, bz), f32),
            pltpu.VMEM((2,) + block, f32),
            pltpu.VMEM((2, EXPAND, by, bz), f32),
            pltpu.VMEM((2, EXPAND, bx, bz), f32),
            pltpu.VMEM((2,) + block, f32),
            pltpu.VMEM((EXPAND, 2, by, bz), f32),
            pltpu.VMEM((EXPAND, 2) + block, f32),
            pltpu.VMEM((EXPAND, 2) + block, f32),
            pltpu.VMEM((2, 8, LANES), f32),
            pltpu.VMEM((n0 - 1, 8, LANES), f32),
            pltpu.VMEM((n1 - 1, 8, LANES), f32),
            pltpu.VMEM((EXPAND, 1, LANES), f32),
            pltpu.VMEM((EXPAND, nrow - 1, 1, LANES), f32),
            pltpu.VMEM((EXPAND, n1 - 1, 1, LANES), f32),
            pltpu.VMEM((EXPAND, 1, LANES), f32),
            dma, dma((24,)), dma((24,)),
            dma((n0 - 1,)), dma((n0 - 1,)), dma((n1 - 1,)), dma((n1 - 1,)),
            dma((EXPAND, nrow - 1)), dma((EXPAND, nrow - 1)),
            dma((EXPAND, n1 - 1)), dma((EXPAND, n1 - 1)),
            pltpu.SemaphoreType.REGULAR,
        ],
        compiler_params=pltpu.CompilerParams(collective_id=0, has_side_effects=True),
    )(krylov_basis, schur_vectors.T, next_vector, diag_shift, velocity)
    return vectors, columns[0:EXPAND, 0:ROWS].T


def solution(mesh):
    in_specs = (
        P(None, "gx", "gy", "gz"),
        P(),
        P("gx", "gy", "gz"),
        P("gx", "gy", "gz"),
        P(None, "gx", "gy", "gz"),
    )
    out_specs = (P(None, "gx", "gy", "gz"), P())
    return jax.shard_map(
        per_device, mesh=mesh, in_specs=in_specs, out_specs=out_specs, check_vma=False
    )
```

```python
import functools

import jax
import jax.numpy as jnp
from jax import lax
from jax.experimental import pallas as pl
from jax.experimental.pallas import tpu as pltpu
from jax.sharding import PartitionSpec as P

KEEP = 20
EXPAND = 3
ROWS = 24
LANES = 128
GROUP = 32
DIRECT = 64
AXES = ("gx", "gy", "gz")


def partner_steps(phase, sizes):
    xs = range(1, sizes[0]) if phase else ()
    steps = [(dx, 0, 0) for dx in xs] if phase == 1 else [
        (dx, dy, dz) for dx in tuple(xs) + (0,)
        for dy in range(sizes[1]) for dz in range(sizes[2])]
    return [step for step in steps if step != (0, 0, 0)]


def body(
    sizes, cells,
    kry_hbm, schur_hbm, w_hbm, diag_hbm, vel_hbm,
    out, hess,
    schur, w_ref, diag, vel, kry, image, xr, yr, zr, ypack, zpack, xh, yh, zh, xs, ys, zs,
    gsend, grecv0, grecv1, rsend, rrecv0, rrecv1, mid,
    load_sem, halo_send, halo_recv, gsem_s0, gsem_r0, gsem_s1, gsem_r1,
    rsem_s0, rsem_r0, rsem_s1, rsem_r1, ready,
):
    place = tuple(lax.axis_index(a) for a in AXES)
    basis = kry.shape[0]
    bx, by, bz = w_ref.shape
    loads = [
        pltpu.make_async_copy(source, target, load_sem.at[k])
        for k, (source, target) in enumerate((
            (w_hbm, w_ref), (schur_hbm, schur), (kry_hbm, kry), (diag_hbm, diag), (vel_hbm, vel)))
    ]
    for copy in loads:
        copy.start()
    direct = sizes[0] * sizes[1] * sizes[2] <= DIRECT
    shifted = [[lax.rem(place[d] + k, sizes[d]) for k in range(sizes[d])] for d in range(3)]

    def partners(phase):
        return [tuple(shifted[d][step[d]] for d in range(3))
                for step in partner_steps(phase, sizes)]


    for ref in (xr, yr, zr, xs, ys, zs):
        ref[...] = jnp.zeros_like(ref)

    barrier = pltpu.get_barrier_semaphore()
    for to in partners(0) + partners(1):
        pl.semaphore_signal(
            barrier, inc=1, device_id=to, device_id_type=pl.DeviceIdType.MESH)
    pl.semaphore_wait(barrier, len(partners(0)) + len(partners(1)))

    def halo_copies(kind, sources, targets):
        found = []
        for d in range(3):
            for side in (0, 1):
                at = (kind * 3 + d) * 2 + side
                to = list(place)
                to[d] = place[d] + (1 if side == 0 else -1)
                can_send = place[d] < sizes[d] - 1 if side == 0 else place[d] > 0
                can_recv = place[d] > 0 if side == 0 else place[d] < sizes[d] - 1
                found.append((
                    pltpu.make_async_remote_copy(
                        src_ref=sources[d][side], dst_ref=targets[d][side],
                        send_sem=halo_send.at[at], recv_sem=halo_recv.at[at],
                        device_id=tuple(to), device_id_type=pl.DeviceIdType.MESH,
                    ), can_send, can_recv))
        return found

    def halo_start(copies):
        for copy, can_send, _ in copies:
            pl.when(can_send)(copy.start)

    def halo_wait(copies):
        for copy, _, can_recv in copies:
            pl.when(can_recv)(copy.wait_recv)

    def halo_finish(copies):
        for copy, can_send, _ in copies:
            pl.when(can_send)(copy.wait_send)

    def field_copies(kind, ref):
        return halo_copies(
            kind,
            ((ref.at[bx - 1], ref.at[0]), (ref, ref), (ref, ref)),
            tuple((r.at[kind, 0], r.at[kind, 1]) for r in (xs, ys, zs)),
        )

    def exchange(send, slots, sems_s, sems_r, phase):
        copies = []
        for at, to in enumerate(partners(phase)):
            copies.append(pltpu.make_async_remote_copy(
                src_ref=send, dst_ref=slots.at[at],
                send_sem=sems_s.at[at], recv_sem=sems_r.at[at],
                device_id=to, device_id_type=pl.DeviceIdType.MESH,
            ))
        for copy in copies:
            copy.start()
        return copies

    def gather_sum(copies, own, slots):
        for copy in copies:
            copy.wait_recv()
        terms = [own] + [slots[k] for k in range(len(copies))]
        while len(terms) > 1:
            terms = [sum(terms[k:k + 2]) for k in range(0, len(terms), 2)]
        return terms[0]

    pending = []

    def row_start(k, rowform):
        rsend[k] = rowform
        phase = 2 if direct else 0
        copies = exchange(rsend.at[k], rrecv0.at[k], rsem_s0.at[k], rsem_r0.at[k], phase)
        pending.append(copies)
        return copies

    def row_end(k, rowform, copies):
        rowform = gather_sum(copies, rowform, rrecv0.at[k])
        if not direct:
            mid[k] = rowform
            copies = exchange(mid.at[k], rrecv1.at[k], rsem_s1.at[k], rsem_r1.at[k], 1)
            pending.append(copies)
            rowform = gather_sum(copies, rowform, rrecv1.at[k])
        return rowform * (1.0 / cells)

    lane3 = lax.broadcasted_iota(jnp.int32, (by, bz), 1)
    row3 = lax.broadcasted_iota(jnp.int32, (by, bz), 0)

    def stencil(v, x_before, x_after, y_before, y_after, z_before, z_after):
        res = []
        for x in range(bx):
            here = v[x]
            xb = v[x - 1] if x > 0 else x_before
            xa = v[x + 1] if x < bx - 1 else x_after
            yb = jnp.where(row3 == 0, y_before[x], pltpu.roll(here, 1, 0))
            ya = jnp.where(row3 == by - 1, y_after[x], pltpu.roll(here, by - 1, 0))
            zb = jnp.where(lane3 == 0, z_before[x], pltpu.roll(here, 1, 1))
            za = jnp.where(lane3 == bz - 1, z_after[x], pltpu.roll(here, bz - 1, 1))
            neighbours = xa + xb + ya + yb + za + zb
            flow = (vel[0, x] * (xa - xb) + vel[1, x] * (ya - yb) + vel[2, x] * (za - zb))
            res.append((6.0 + diag[x]) * here - neighbours + 0.5 * flow)
        return res

    def dots(v, count):
        parts = []
        for i in range(ROWS):
            if i < count:
                total = out[i, 0] * v[0]
                for x in range(1, bx):
                    total = total + out[i, x] * v[x]
            elif i == ROWS - 1:
                total = v[0] * v[0]
                for x in range(1, bx):
                    total = total + v[x] * v[x]
            else:
                total = None
            parts.append(jnp.zeros((1, bz), jnp.float32) if total is None
                         else jnp.sum(total, axis=0, keepdims=True))
        return jnp.sum(jnp.concatenate(parts, axis=0), axis=1, keepdims=True)

    halo_w = field_copies(0, w_ref)
    loads[0].wait()
    halo_start(halo_w)
    if direct:
        for to in partners(1):
            pl.semaphore_signal(
                ready, inc=1, device_id=to, device_id_type=pl.DeviceIdType.MESH)

    out[KEEP + 1:ROWS] = jnp.zeros((ROWS - KEEP - 1, bx, by, bz), jnp.float32)
    out[KEEP] = w_ref[...]
    loads[1].wait()
    loads[2].wait()
    wide, deep = 5, 4
    for first in range(0, KEEP, wide):
        def step(at, sums, first=first):
            sums = list(sums)
            for k in range(deep):
                i = at * deep + k
                for x in range(bx):
                    tile = kry[i, x]
                    for j in range(wide):
                        sums[j * bx + x] = sums[j * bx + x] + schur[first + j, i] * tile
            return tuple(sums)
        sums = lax.fori_loop(
            0, basis // deep, step,
            tuple(jnp.zeros((by, bz), jnp.float32) for _ in range(wide * bx)))
        for j in range(wide):
            for x in range(bx):
                out[first + j, x] = sums[j * bx + x]

    for side, (row, edge) in enumerate(((by - 1, bz - 1), (0, 0))):
        for i in range(KEEP):
            ypack[side, i] = out[i, :, row, :]
        for x in range(bx):
            packed = jnp.zeros((by, bz), jnp.float32)
            for i in range(KEEP):
                packed = jnp.where(
                    lane3 == i, pltpu.roll(out[i, x], (i - edge) % bz, 1), packed)
            zpack[side, x] = packed
    halo_r = halo_copies(
        3,
        ((out.at[0:KEEP, bx - 1], out.at[0:KEEP, 0]), (ypack.at[0], ypack.at[1]),
         (zpack.at[0], zpack.at[1])),
        tuple((r.at[0], r.at[1]) for r in (xr, yr, zr)),
    )
    halo_start(halo_r)

    row = lax.broadcasted_iota(jnp.int32, (ROWS, LANES), 0)
    lane = lax.broadcasted_iota(jnp.int32, (ROWS, LANES), 1)
    lane1 = lax.broadcasted_iota(jnp.int32, (1, LANES), 1)
    row1 = lax.broadcasted_iota(jnp.int32, (ROWS, 1), 0)

    gram = jnp.zeros((ROWS, LANES), jnp.float32)
    for j in range(KEEP + 1):
        col = dots([out[j, x] for x in range(bx)], KEEP + 1)
        gram = jnp.where(lane == j, jnp.where(row < KEEP + 1, col, 0.0), gram)

    packed = jnp.zeros((8, LANES), jnp.float32)
    for part in range(ROWS // 8):
        piece = gram[part * 8:part * 8 + 8]
        packed = packed + (pltpu.roll(piece, part * GROUP, 1) if part else piece)
    gsend[0] = packed
    gcopies0 = exchange(gsend.at[0], grecv0, gsem_s0, gsem_r0, 0)

    loads[3].wait()
    loads[4].wait()
    halo_wait(halo_w)
    applied = stencil(
        [w_ref[x] for x in range(bx)], xs[0, 0], xs[0, 1],
        [ys[0, 0, x, by - 1:by, :] for x in range(bx)],
        [ys[0, 1, x, 0:1, :] for x in range(bx)],
        [zs[0, 0, x, :, bz - 1:bz] for x in range(bx)],
        [zs[0, 1, x, :, 0:1] for x in range(bx)],
    )
    for x in range(bx):
        image[0, x] = applied[x]
    ownrow = jnp.sum(jnp.where(row == lane, dots(applied, KEEP + 1), 0.0),
                     axis=0, keepdims=True)
    if direct:
        pl.semaphore_wait(ready, sizes[0] - 1)
    copies = row_start(0, ownrow)
    halo_a = field_copies(1, image.at[0])
    halo_start(halo_a)

    packed = gather_sum(gcopies0, packed, grecv0)
    gsend[1] = packed
    gcopies1 = exchange(gsend.at[1], grecv1, gsem_s1, gsem_r1, 1)
    packed = gather_sum(gcopies1, packed, grecv1) * (1.0 / cells)
    pending += [gcopies0, gcopies1]
    gram = jnp.concatenate(
        [packed] + [pltpu.roll(packed, LANES - part * GROUP, 1) for part in range(1, ROWS // 8)],
        axis=0)
    gram = jnp.where((lane < KEEP + 1) & (row < KEEP + 1), gram, 0.0)
    norm_sq = jnp.sum(
        jnp.sum(jnp.where((lane == KEEP) & (row == KEEP), gram, 0.0), axis=1, keepdims=True),
        axis=0, keepdims=True)
    scale = 1.0 / jnp.maximum(jnp.sqrt(norm_sq), 0.5)
    gram = gram * jnp.where(row == KEEP, scale, 1.0) * jnp.where(lane == KEEP, scale, 1.0)
    for x in range(bx):
        out[KEEP, x] = w_ref[x] * scale
    applied = [tile * scale for tile in applied]
    rowform = row_end(0, ownrow, copies)
    rowform = rowform * scale * jnp.where((lane1 == KEEP) | (lane1 == ROWS - 1), scale, 1.0)

    halo_wait(halo_r)
    for side in (0, 1):
        near_row, near_lane = (by - 1, bz - 1) if side == 0 else (0, 0)
        xh[side, 0] = xs[0, side] * scale
        for x in range(bx):
            yh[side, 0, x:x + 1] = ys[0, side, x, near_row:near_row + 1, :] * scale
            zh[side, x] = jnp.where(
                lane3 == KEEP, zs[0, side, x, :, near_lane:near_lane + 1] * scale, zr[side, x])
    halos = {1: halo_a}
    hcols = []
    for k in range(EXPAND):
        count = KEEP + 1 + k
        if k > 0:
            rowform = jnp.sum(jnp.where(row == lane, dots(applied, count), 0.0),
                              axis=0, keepdims=True)
            rowform = row_end(k, rowform, row_start(k, rowform))
        c_row = jnp.where(lane1 < count, rowform, 0.0)
        twice = jnp.where(row == lane, 2.0, 0.0) - gram
        t_col = jnp.sum(twice * c_row, axis=1, keepdims=True)
        weights = jnp.broadcast_to(t_col, (ROWS, LANES))
        t_row = jnp.sum(jnp.where(row == lane, weights, 0.0), axis=0, keepdims=True)
        gt_row = jnp.sum(gram * weights, axis=0, keepdims=True)
        length_sq = jnp.sum(
            jnp.where(lane1 == ROWS - 1, rowform, t_row * (gt_row - 2.0 * c_row)),
            axis=1, keepdims=True)
        length_sq = jnp.maximum(length_sq, 0.0)
        length = jnp.sqrt(length_sq)
        inverse = 1.0 / jnp.maximum(length, 0.5)
        hcols.append(jnp.where(lane1 == count, length, t_row))
        newest = list(applied)
        for i in range(count):
            weight = jnp.broadcast_to(weights[i:i + 1, :], (by, bz))
            for x in range(bx):
                newest[x] = newest[x] - weight * out[i, x]
        newest = [tile * inverse for tile in newest]
        for x in range(bx):
            out[count, x] = newest[x]
        if k == EXPAND - 1:
            break
        halo_wait(halos[k + 1])
        sides = []
        for side in (0, 1):
            near_row, near_lane = (by - 1, bz - 1) if side == 0 else (0, 0)
            factor = scale if k == 0 else 1.0
            x_part = xs[k + 1, side] * factor
            y_part = [ys[k + 1, side, x, near_row:near_row + 1, :] * factor for x in range(bx)]
            y_part = jnp.concatenate(y_part, axis=0)
            for i in range(count):
                weight = weights[i:i + 1, :]
                if i < KEEP:
                    x_part = x_part - weight * xr[side, i]
                    y_part = y_part - weight * yr[side, i]
                else:
                    x_part = x_part - weight * xh[side, i - KEEP]
                    y_part = y_part - weight * yh[side, i - KEEP]
            x_part = x_part * inverse
            y_part = y_part * inverse
            z_part = []
            for x in range(bx):
                column = (zs[k + 1, side, x, :, near_lane:near_lane + 1] * factor
                          - jnp.sum(zh[side, x] * t_row, axis=1, keepdims=True)) * inverse
                z_part.append(column)
                if k + 1 < EXPAND - 1:
                    zh[side, x] = jnp.where(lane3 == count, column, zh[side, x])
            xh[side, count - KEEP] = x_part
            yh[side, count - KEEP] = y_part
            sides.append((x_part, [y_part[x:x + 1] for x in range(bx)], z_part))
        applied = stencil(newest, sides[0][0], sides[1][0], sides[0][1], sides[1][1],
                          sides[0][2], sides[1][2])
        if k + 1 < EXPAND - 1:
            for x in range(bx):
                image[1, x] = applied[x]
            halos[k + 2] = field_copies(k + 2, image.at[1])
            halo_start(halos[k + 2])
        e_row = t_row - c_row
        e_col = jnp.sum(jnp.where(row == lane, e_row, 0.0), axis=1, keepdims=True)
        cross_col = (e_col - jnp.sum(gram * e_row, axis=1, keepdims=True)) * inverse
        cross_row = (e_row - jnp.sum(gram * e_col, axis=0, keepdims=True)) * inverse
        corner = length_sq * inverse * inverse
        gram = jnp.where(row == count, cross_row, jnp.where(lane == count, cross_col, gram))
        gram = jnp.where((row == count) & (lane == count), corner, gram)

    for k in range(EXPAND):
        hess[k:k + 1] = hcols[k % len(hcols)]
    halo_finish(halo_w)
    halo_finish(halo_r)
    for copies in halos.values():
        halo_finish(copies)
    for copies in pending:
        for copy in copies:
            copy.wait_send()


def per_device(krylov_basis, schur_vectors, next_vector, diag_shift, velocity):
    sizes = tuple(lax.axis_size(a) for a in AXES)
    block = next_vector.shape
    bx, by, bz = block
    cells = float(bx * by * bz * sizes[0] * sizes[1] * sizes[2])
    n0, n1 = sizes[1] * sizes[2], sizes[0]
    nrow = n0 * n1 if n0 * n1 <= DIRECT else n0
    f32 = jnp.float32
    vmem = pl.BlockSpec(memory_space=pltpu.VMEM)
    dma = pltpu.SemaphoreType.DMA
    vectors, columns = pl.pallas_call(
        functools.partial(body, sizes, cells),
        out_shape=(
            pltpu.VMEM((ROWS,) + block, f32),
            pltpu.VMEM((8, LANES), f32),
        ),
        in_specs=[
            pl.BlockSpec(memory_space=pl.ANY) for _ in range(5)
        ],
        out_specs=(vmem, vmem),
        scratch_shapes=[
            pltpu.SMEM(schur_vectors.shape[::-1], f32),
            pltpu.VMEM(block, f32),
            pltpu.VMEM(block, f32),
            pltpu.VMEM((3,) + block, f32),
            pltpu.VMEM(krylov_basis.shape, f32),
            pltpu.VMEM((2,) + block, f32),
            pltpu.VMEM((2, KEEP, by, bz), f32),
            pltpu.VMEM((2, KEEP, bx, bz), f32),
            pltpu.VMEM((2,) + block, f32),
            pltpu.VMEM((2, KEEP, bx, bz), f32),
            pltpu.VMEM((2,) + block, f32),
            pltpu.VMEM((2, EXPAND, by, bz), f32),
            pltpu.VMEM((2, EXPAND, bx, bz), f32),
            pltpu.VMEM((2,) + block, f32),
            pltpu.VMEM((EXPAND, 2, by, bz), f32),
            pltpu.VMEM((EXPAND, 2) + block, f32),
            pltpu.VMEM((EXPAND, 2) + block, f32),
            pltpu.VMEM((2, 8, LANES), f32),
            pltpu.VMEM((n0 - 1, 8, LANES), f32),
            pltpu.VMEM((n1 - 1, 8, LANES), f32),
            pltpu.VMEM((EXPAND, 1, LANES), f32),
            pltpu.VMEM((EXPAND, nrow - 1, 1, LANES), f32),
            pltpu.VMEM((EXPAND, n1 - 1, 1, LANES), f32),
            pltpu.VMEM((EXPAND, 1, LANES), f32),
            dma((5,)), dma((24,)), dma((24,)),
            dma((n0 - 1,)), dma((n0 - 1,)), dma((n1 - 1,)), dma((n1 - 1,)),
            dma((EXPAND, nrow - 1)), dma((EXPAND, nrow - 1)),
            dma((EXPAND, n1 - 1)), dma((EXPAND, n1 - 1)),
            pltpu.SemaphoreType.REGULAR,
        ],
        compiler_params=pltpu.CompilerParams(collective_id=0, has_side_effects=True),
    )(krylov_basis, schur_vectors.T, next_vector, diag_shift, velocity)
    return vectors, columns[0:EXPAND, 0:ROWS].T


def solution(mesh):
    in_specs = (
        P(None, "gx", "gy", "gz"),
        P(),
        P("gx", "gy", "gz"),
        P("gx", "gy", "gz"),
        P(None, "gx", "gy", "gz"),
    )
    out_specs = (P(None, "gx", "gy", "gz"), P())
    return jax.shard_map(
        per_device, mesh=mesh, in_specs=in_specs, out_specs=out_specs, check_vma=False
    )
```

```python
import functools

import jax
import jax.numpy as jnp
from jax import lax
from jax.experimental import pallas as pl
from jax.experimental.pallas import tpu as pltpu
from jax.sharding import PartitionSpec as P

KEEP = 20
EXPAND = 3
ROWS = 24
LANES = 128
GROUP = 32
DIRECT = 64
AXES = ("gx", "gy", "gz")


def partner_steps(phase, sizes):
    xs = range(1, sizes[0]) if phase else ()
    steps = [(dx, 0, 0) for dx in xs] if phase == 1 else [
        (dx, dy, dz) for dx in tuple(reversed(xs)) + (0,)
        for dy in range(sizes[1]) for dz in range(sizes[2])]
    return [step for step in steps if step != (0, 0, 0)]


def body(
    sizes, cells,
    kry_hbm, schur_hbm, w_hbm, diag_hbm, vel_hbm,
    out, hess,
    schur, w_ref, diag, vel, kry, image, xr, yr, zr, ypack, zpack, xh, yh, zh, xs, ys, zs,
    gsend, grecv0, grecv1, rsend, rrecv0, rrecv1, mid,
    load_sem, halo_send, halo_recv, gsem_s0, gsem_r0, gsem_s1, gsem_r1,
    rsem_s0, rsem_r0, rsem_s1, rsem_r1, ready,
):
    place = tuple(lax.axis_index(a) for a in AXES)
    basis = kry.shape[0]
    bx, by, bz = w_ref.shape
    loads = [
        pltpu.make_async_copy(source, target, load_sem.at[k])
        for k, (source, target) in enumerate((
            (w_hbm, w_ref), (schur_hbm, schur), (kry_hbm, kry), (diag_hbm, diag), (vel_hbm, vel)))
    ]
    for copy in loads:
        copy.start()
    direct = sizes[0] * sizes[1] * sizes[2] <= DIRECT
    shifted = [[lax.rem(place[d] + k, sizes[d]) for k in range(sizes[d])] for d in range(3)]

    def partners(phase):
        return [tuple(shifted[d][step[d]] for d in range(3))
                for step in partner_steps(phase, sizes)]


    for ref in (xr, yr, zr, xs, ys, zs):
        ref[...] = jnp.zeros_like(ref)

    barrier = pltpu.get_barrier_semaphore()
    for to in partners(0) + partners(1):
        pl.semaphore_signal(
            barrier, inc=1, device_id=to, device_id_type=pl.DeviceIdType.MESH)
    pl.semaphore_wait(barrier, len(partners(0)) + len(partners(1)))

    def halo_copies(kind, sources, targets):
        found = []
        for d in range(3):
            for side in (0, 1):
                at = (kind * 3 + d) * 2 + side
                to = list(place)
                to[d] = place[d] + (1 if side == 0 else -1)
                can_send = place[d] < sizes[d] - 1 if side == 0 else place[d] > 0
                can_recv = place[d] > 0 if side == 0 else place[d] < sizes[d] - 1
                found.append((
                    pltpu.make_async_remote_copy(
                        src_ref=sources[d][side], dst_ref=targets[d][side],
                        send_sem=halo_send.at[at], recv_sem=halo_recv.at[at],
                        device_id=tuple(to), device_id_type=pl.DeviceIdType.MESH,
                    ), can_send, can_recv))
        return found

    def halo_start(copies):
        for copy, can_send, _ in copies:
            pl.when(can_send)(copy.start)

    def halo_wait(copies):
        for copy, _, can_recv in copies:
            pl.when(can_recv)(copy.wait_recv)

    def halo_finish(copies):
        for copy, can_send, _ in copies:
            pl.when(can_send)(copy.wait_send)

    def field_copies(kind, ref):
        return halo_copies(
            kind,
            ((ref.at[bx - 1], ref.at[0]), (ref, ref), (ref, ref)),
            tuple((r.at[kind, 0], r.at[kind, 1]) for r in (xs, ys, zs)),
        )

    def exchange(send, slots, sem_s, sem_r, phase):
        for at, to in enumerate(partners(phase)):
            pltpu.make_async_remote_copy(
                src_ref=send, dst_ref=slots.at[at], send_sem=sem_s, recv_sem=sem_r,
                device_id=to, device_id_type=pl.DeviceIdType.MESH,
            ).start()
        pending.append(pltpu.make_async_copy(slots, slots, sem_s))
        return pltpu.make_async_copy(slots, slots, sem_r)

    def gather_sum(arrival, own, slots):
        arrival.wait()
        terms = [own] + [slots[k] for k in range(slots.shape[0])]
        while len(terms) > 1:
            terms = [sum(terms[k + 1:k + 2], terms[k]) for k in range(0, len(terms), 2)]
        return terms[0]

    pending = []

    def finish_sends():
        while pending:
            pending.pop().wait()

    def row_start(k, rowform):
        rsend[k] = rowform
        return exchange(rsend.at[k], rrecv0.at[k], rsem_s0.at[k], rsem_r0.at[k],
                        2 if direct else 0)

    def row_end(k, rowform, arrival):
        rowform = gather_sum(arrival, rowform, rrecv0.at[k])
        if not direct:
            mid[k] = rowform
            arrival = exchange(mid.at[k], rrecv1.at[k], rsem_s1.at[k], rsem_r1.at[k], 1)
            rowform = gather_sum(arrival, rowform, rrecv1.at[k])
        return rowform * (1.0 / cells)

    lane3 = lax.broadcasted_iota(jnp.int32, (by, bz), 1)
    row3 = lax.broadcasted_iota(jnp.int32, (by, bz), 0)

    def stencil(v, x_before, x_after, y_before, y_after, z_before, z_after):
        res = []
        for x in range(bx):
            here = v[x]
            xb = v[x - 1] if x > 0 else x_before
            xa = v[x + 1] if x < bx - 1 else x_after
            yb = jnp.where(row3 == 0, y_before[x], pltpu.roll(here, 1, 0))
            ya = jnp.where(row3 == by - 1, y_after[x], pltpu.roll(here, by - 1, 0))
            zb = jnp.where(lane3 == 0, z_before[x], pltpu.roll(here, 1, 1))
            za = jnp.where(lane3 == bz - 1, z_after[x], pltpu.roll(here, bz - 1, 1))
            neighbours = xa + xb + ya + yb + za + zb
            flow = (vel[0, x] * (xa - xb) + vel[1, x] * (ya - yb) + vel[2, x] * (za - zb))
            res.append((6.0 + diag[x]) * here - neighbours + 0.5 * flow)
        return res

    def dots(v, count):
        parts = []
        for i in range(ROWS):
            if i < count:
                total = out[i, 0] * v[0]
                for x in range(1, bx):
                    total = total + out[i, x] * v[x]
            elif i == ROWS - 1:
                total = v[0] * v[0]
                for x in range(1, bx):
                    total = total + v[x] * v[x]
            else:
                total = None
            parts.append(jnp.zeros((1, bz), jnp.float32) if total is None
                         else jnp.sum(total, axis=0, keepdims=True))
        return jnp.sum(jnp.concatenate(parts, axis=0), axis=1, keepdims=True)

    halo_w = field_copies(0, w_ref)
    loads[0].wait()
    halo_start(halo_w)
    if direct:
        for to in partners(1):
            pl.semaphore_signal(
                ready, inc=1, device_id=to, device_id_type=pl.DeviceIdType.MESH)

    out[KEEP + 1:ROWS] = jnp.zeros((ROWS - KEEP - 1, bx, by, bz), jnp.float32)
    out[KEEP] = w_ref[...]
    loads[1].wait()
    loads[2].wait()
    wide, deep = 5, 4
    for first in range(0, KEEP, wide):
        def step(at, sums, first=first):
            sums = list(sums)
            for k in range(deep):
                i = at * deep + k
                for x in range(bx):
                    tile = kry[i, x]
                    for j in range(wide):
                        sums[j * bx + x] = sums[j * bx + x] + schur[first + j, i] * tile
            return tuple(sums)
        sums = lax.fori_loop(
            0, basis // deep, step,
            tuple(jnp.zeros((by, bz), jnp.float32) for _ in range(wide * bx)))
        for j in range(wide):
            for x in range(bx):
                out[first + j, x] = sums[j * bx + x]

    for side, (row, edge) in enumerate(((by - 1, bz - 1), (0, 0))):
        for i in range(KEEP):
            ypack[side, i] = out[i, :, row, :]
        for x in range(bx):
            packed = jnp.zeros((by, bz), jnp.float32)
            for i in range(KEEP):
                packed = jnp.where(
                    lane3 == i, pltpu.roll(out[i, x], (i - edge) % bz, 1), packed)
            zpack[side, x] = packed
    halo_r = halo_copies(
        3,
        ((out.at[0:KEEP, bx - 1], out.at[0:KEEP, 0]), (ypack.at[0], ypack.at[1]),
         (zpack.at[0], zpack.at[1])),
        tuple((r.at[0], r.at[1]) for r in (xr, yr, zr)),
    )
    halo_start(halo_r)

    row = lax.broadcasted_iota(jnp.int32, (ROWS, LANES), 0)
    lane = lax.broadcasted_iota(jnp.int32, (ROWS, LANES), 1)
    lane1 = lax.broadcasted_iota(jnp.int32, (1, LANES), 1)
    row1 = lax.broadcasted_iota(jnp.int32, (ROWS, 1), 0)

    gram = jnp.zeros((ROWS, LANES), jnp.float32)
    for j in range(KEEP + 1):
        col = dots([out[j, x] for x in range(bx)], KEEP + 1)
        gram = jnp.where(lane == j, jnp.where(row < KEEP + 1, col, 0.0), gram)

    packed = jnp.zeros((8, LANES), jnp.float32)
    for part in range(ROWS // 8):
        piece = gram[part * 8:part * 8 + 8]
        packed = packed + (pltpu.roll(piece, part * GROUP, 1) if part else piece)
    gsend[0] = packed
    arrival0 = exchange(gsend.at[0], grecv1, gsem_s1, gsem_r1, 1)

    loads[3].wait()
    loads[4].wait()
    halo_wait(halo_w)
    applied = stencil(
        [w_ref[x] for x in range(bx)], xs[0, 0], xs[0, 1],
        [ys[0, 0, x, by - 1:by, :] for x in range(bx)],
        [ys[0, 1, x, 0:1, :] for x in range(bx)],
        [zs[0, 0, x, :, bz - 1:bz] for x in range(bx)],
        [zs[0, 1, x, :, 0:1] for x in range(bx)],
    )
    for x in range(bx):
        image[0, x] = applied[x]
    ownrow = jnp.sum(jnp.where(row == lane, dots(applied, KEEP + 1), 0.0),
                     axis=0, keepdims=True)
    if direct:
        pl.semaphore_wait(ready, sizes[0] - 1)
    copies = row_start(0, ownrow)
    halo_a = field_copies(1, image.at[0])
    halo_start(halo_a)

    packed = gather_sum(arrival0, packed, grecv1)
    gsend[1] = packed
    arrival1 = exchange(gsend.at[1], grecv0, gsem_s0, gsem_r0, 0)
    packed = gather_sum(arrival1, packed, grecv0) * (1.0 / cells)
    gram = jnp.concatenate(
        [packed] + [pltpu.roll(packed, LANES - part * GROUP, 1) for part in range(1, ROWS // 8)],
        axis=0)
    gram = jnp.where((lane < KEEP + 1) & (row < KEEP + 1), gram, 0.0)
    norm_sq = jnp.sum(
        jnp.sum(jnp.where((lane == KEEP) & (row == KEEP), gram, 0.0), axis=1, keepdims=True),
        axis=0, keepdims=True)
    scale = 1.0 / jnp.maximum(jnp.sqrt(norm_sq), 0.5)
    gram = gram * jnp.where(row == KEEP, scale, 1.0) * jnp.where(lane == KEEP, scale, 1.0)
    for x in range(bx):
        out[KEEP, x] = w_ref[x] * scale
    applied = [tile * scale for tile in applied]
    rowform = row_end(0, ownrow, copies)
    rowform = rowform * scale * jnp.where((lane1 == KEEP) | (lane1 == ROWS - 1), scale, 1.0)

    halo_wait(halo_r)
    for side in (0, 1):
        near_row, near_lane = (by - 1, bz - 1) if side == 0 else (0, 0)
        xh[side, 0] = xs[0, side] * scale
        for x in range(bx):
            yh[side, 0, x:x + 1] = ys[0, side, x, near_row:near_row + 1, :] * scale
            zh[side, x] = jnp.where(
                lane3 == KEEP, zs[0, side, x, :, near_lane:near_lane + 1] * scale, zr[side, x])
    halos = {1: halo_a}
    done = [halo_w, halo_r, halo_a]
    hcols = []
    for k in range(EXPAND):
        count = KEEP + 1 + k
        if k > 0:
            rowform = jnp.sum(jnp.where(row == lane, dots(applied, count), 0.0),
                              axis=0, keepdims=True)
            earlier = pending[:]
            pending.clear()
            arrival = row_start(k, rowform)
            for copy in earlier:
                copy.wait()
            for copies in done:
                halo_finish(copies)
            done = []
            rowform = row_end(k, rowform, arrival)
        c_row = jnp.where(lane1 < count, rowform, 0.0)
        twice = jnp.where(row == lane, 2.0, 0.0) - gram
        t_col = jnp.sum(twice * c_row, axis=1, keepdims=True)
        weights = jnp.broadcast_to(t_col, (ROWS, LANES))
        t_row = jnp.sum(jnp.where(row == lane, weights, 0.0), axis=0, keepdims=True)
        gt_row = jnp.sum(gram * weights, axis=0, keepdims=True)
        length_sq = jnp.sum(
            jnp.where(lane1 == ROWS - 1, rowform, t_row * (gt_row - 2.0 * c_row)),
            axis=1, keepdims=True)
        length_sq = jnp.maximum(length_sq, 0.0)
        length = jnp.sqrt(length_sq)
        inverse = 1.0 / jnp.maximum(length, 0.5)
        hcols.append(jnp.where(lane1 == count, length, t_row))
        newest = list(applied)
        for i in range(count):
            weight = jnp.broadcast_to(weights[i:i + 1, :], (by, bz))
            for x in range(bx):
                newest[x] = newest[x] - weight * out[i, x]
        newest = [tile * inverse for tile in newest]
        for x in range(bx):
            out[count, x] = newest[x]
        if k == EXPAND - 1:
            break
        halo_wait(halos[k + 1])
        sides = []
        for side in (0, 1):
            near_row, near_lane = (by - 1, bz - 1) if side == 0 else (0, 0)
            factor = scale if k == 0 else 1.0
            x_part = xs[k + 1, side] * factor
            y_part = [ys[k + 1, side, x, near_row:near_row + 1, :] * factor for x in range(bx)]
            y_part = jnp.concatenate(y_part, axis=0)
            for i in range(count):
                weight = weights[i:i + 1, :]
                if i < KEEP:
                    x_part = x_part - weight * xr[side, i]
                    y_part = y_part - weight * yr[side, i]
                else:
                    x_part = x_part - weight * xh[side, i - KEEP]
                    y_part = y_part - weight * yh[side, i - KEEP]
            x_part = x_part * inverse
            y_part = y_part * inverse
            z_part = []
            for x in range(bx):
                column = (zs[k + 1, side, x, :, near_lane:near_lane + 1] * factor
                          - jnp.sum(zh[side, x] * t_row, axis=1, keepdims=True)) * inverse
                z_part.append(column)
                if k + 1 < EXPAND - 1:
                    zh[side, x] = jnp.where(lane3 == count, column, zh[side, x])
            xh[side, count - KEEP] = x_part
            yh[side, count - KEEP] = y_part
            sides.append((x_part, [y_part[x:x + 1] for x in range(bx)], z_part))
        applied = stencil(newest, sides[0][0], sides[1][0], sides[0][1], sides[1][1],
                          sides[0][2], sides[1][2])
        if k + 1 < EXPAND - 1:
            for x in range(bx):
                image[1, x] = applied[x]
            halos[k + 2] = field_copies(k + 2, image.at[1])
            halo_start(halos[k + 2])
            done.append(halos[k + 2])
        e_row = t_row - c_row
        e_col = jnp.sum(jnp.where(row == lane, e_row, 0.0), axis=1, keepdims=True)
        cross_col = (e_col - jnp.sum(gram * e_row, axis=1, keepdims=True)) * inverse
        cross_row = (e_row - jnp.sum(gram * e_col, axis=0, keepdims=True)) * inverse
        corner = length_sq * inverse * inverse
        gram = jnp.where(row == count, cross_row, jnp.where(lane == count, cross_col, gram))
        gram = jnp.where((row == count) & (lane == count), corner, gram)

    for k in range(EXPAND):
        hess[k:k + 1] = hcols[k % len(hcols)]
    for copies in done:
        halo_finish(copies)
    finish_sends()


def per_device(krylov_basis, schur_vectors, next_vector, diag_shift, velocity):
    sizes = tuple(lax.axis_size(a) for a in AXES)
    block = next_vector.shape
    bx, by, bz = block
    cells = float(bx * by * bz * sizes[0] * sizes[1] * sizes[2])
    n0, n1 = sizes[1] * sizes[2], sizes[0]
    nrow = n0 * n1 if n0 * n1 <= DIRECT else n0
    f32 = jnp.float32
    vmem = pl.BlockSpec(memory_space=pltpu.VMEM)
    dma = pltpu.SemaphoreType.DMA
    vectors, columns = pl.pallas_call(
        functools.partial(body, sizes, cells),
        out_shape=(
            pltpu.VMEM((ROWS,) + block, f32),
            pltpu.VMEM((8, LANES), f32),
        ),
        in_specs=[
            pl.BlockSpec(memory_space=pl.ANY) for _ in range(5)
        ],
        out_specs=(vmem, vmem),
        scratch_shapes=[
            pltpu.SMEM(schur_vectors.shape[::-1], f32),
            pltpu.VMEM(block, f32),
            pltpu.VMEM(block, f32),
            pltpu.VMEM((3,) + block, f32),
            pltpu.VMEM(krylov_basis.shape, f32),
            pltpu.VMEM((2,) + block, f32),
            pltpu.VMEM((2, KEEP, by, bz), f32),
            pltpu.VMEM((2, KEEP, bx, bz), f32),
            pltpu.VMEM((2,) + block, f32),
            pltpu.VMEM((2, KEEP, bx, bz), f32),
            pltpu.VMEM((2,) + block, f32),
            pltpu.VMEM((2, EXPAND, by, bz), f32),
            pltpu.VMEM((2, EXPAND, bx, bz), f32),
            pltpu.VMEM((2,) + block, f32),
            pltpu.VMEM((EXPAND, 2, by, bz), f32),
            pltpu.VMEM((EXPAND, 2) + block, f32),
            pltpu.VMEM((EXPAND, 2) + block, f32),
            pltpu.VMEM((2, 8, LANES), f32),
            pltpu.VMEM((n0 - 1, 8, LANES), f32),
            pltpu.VMEM((n1 - 1, 8, LANES), f32),
            pltpu.VMEM((EXPAND, 1, LANES), f32),
            pltpu.VMEM((EXPAND, nrow - 1, 1, LANES), f32),
            pltpu.VMEM((EXPAND, n1 - 1, 1, LANES), f32),
            pltpu.VMEM((EXPAND, 1, LANES), f32),
            dma((5,)), dma((24,)), dma((24,)),
            dma, dma, dma, dma,
            dma((EXPAND,)), dma((EXPAND,)), dma((EXPAND,)), dma((EXPAND,)),
            pltpu.SemaphoreType.REGULAR,
        ],
        compiler_params=pltpu.CompilerParams(collective_id=0, has_side_effects=True),
    )(krylov_basis, schur_vectors.T, next_vector, diag_shift, velocity)
    return vectors, columns[0:EXPAND, 0:ROWS].T


def solution(mesh):
    in_specs = (
        P(None, "gx", "gy", "gz"),
        P(),
        P("gx", "gy", "gz"),
        P("gx", "gy", "gz"),
        P(None, "gx", "gy", "gz"),
    )
    out_specs = (P(None, "gx", "gy", "gz"), P())
    return jax.shard_map(
        per_device, mesh=mesh, in_specs=in_specs, out_specs=out_specs, check_vma=False
    )
```

```python
import functools

import jax
import jax.numpy as jnp
from jax import lax
from jax.experimental import pallas as pl
from jax.experimental.pallas import tpu as pltpu
from jax.sharding import PartitionSpec as P

KEEP = 20
EXPAND = 3
ROWS = 24
LANES = 128
UNIT = 16
DIRECT = 64
AXES = ("gx", "gy", "gz")


def partner_steps(phase, sizes):
    xs = range(1, sizes[0]) if phase else ()
    steps = [(dx, 0, 0) for dx in xs] if phase == 1 else [
        (dx, dy, dz) for dx in tuple(reversed(xs)) + (0,)
        for dy in range(sizes[1]) for dz in range(sizes[2])]
    return [step for step in steps if step != (0, 0, 0)]


def body(
    sizes, cells,
    kry_hbm, schur_hbm, w_hbm, diag_hbm, vel_hbm,
    out, hess,
    schur, w_ref, diag, vel, kry, image, xr, yr, zr, ypack, zpack, xh, yh, zh, xs, ys, zs,
    gsend, grecv0, grecv1, rsend, rrecv0, rrecv1, mid,
    load_sem, halo_send, halo_recv, gsem_s0, gsem_r0, gsem_s1, gsem_r1,
    rsem_s0, rsem_r0, rsem_s1, rsem_r1, ready,
):
    place = tuple(lax.axis_index(a) for a in AXES)
    basis = kry.shape[0]
    bx, by, bz = w_ref.shape
    loads = [
        pltpu.make_async_copy(source, target, load_sem.at[k])
        for k, (source, target) in enumerate((
            (w_hbm, w_ref), (schur_hbm, schur), (kry_hbm, kry), (diag_hbm, diag), (vel_hbm, vel)))
    ]
    for copy in loads:
        copy.start()
    direct = sizes[0] * sizes[1] * sizes[2] <= DIRECT
    shifted = [[lax.rem(place[d] + k, sizes[d]) for k in range(sizes[d])] for d in range(3)]

    def partners(phase):
        return [tuple(shifted[d][step[d]] for d in range(3))
                for step in partner_steps(phase, sizes)]


    for ref in (xr, yr, zr, xs, ys, zs):
        ref[...] = jnp.zeros_like(ref)

    barrier = pltpu.get_barrier_semaphore()
    for to in partners(0) + partners(1):
        pl.semaphore_signal(
            barrier, inc=1, device_id=to, device_id_type=pl.DeviceIdType.MESH)
    pl.semaphore_wait(barrier, len(partners(0)) + len(partners(1)))

    def halo_copies(kind, sources, targets):
        found = []
        for d in range(3):
            for side in (0, 1):
                at = (kind * 3 + d) * 2 + side
                to = list(place)
                to[d] = place[d] + (1 if side == 0 else -1)
                can_send = place[d] < sizes[d] - 1 if side == 0 else place[d] > 0
                can_recv = place[d] > 0 if side == 0 else place[d] < sizes[d] - 1
                found.append((
                    pltpu.make_async_remote_copy(
                        src_ref=sources[d][side], dst_ref=targets[d][side],
                        send_sem=halo_send.at[at], recv_sem=halo_recv.at[at],
                        device_id=tuple(to), device_id_type=pl.DeviceIdType.MESH,
                    ), can_send, can_recv))
        return found

    def halo_start(copies):
        for copy, can_send, _ in copies:
            pl.when(can_send)(copy.start)

    def halo_wait(copies):
        for copy, _, can_recv in copies:
            pl.when(can_recv)(copy.wait_recv)

    def halo_finish(copies):
        for copy, can_send, _ in copies:
            pl.when(can_send)(copy.wait_send)

    def field_copies(kind, ref):
        return halo_copies(
            kind,
            ((ref.at[bx - 1], ref.at[0]), (ref, ref), (ref, ref)),
            tuple((r.at[kind, 0], r.at[kind, 1]) for r in (xs, ys, zs)),
        )

    def exchange(send, slots, sem_s, sem_r, phase):
        for at, to in enumerate(partners(phase)):
            pltpu.make_async_remote_copy(
                src_ref=send, dst_ref=slots.at[at], send_sem=sem_s, recv_sem=sem_r,
                device_id=to, device_id_type=pl.DeviceIdType.MESH,
            ).start()
        pending.append(pltpu.make_async_copy(slots, slots, sem_s))
        return pltpu.make_async_copy(slots, slots, sem_r)

    def gather_sum(arrival, own, slots):
        arrival.wait()
        terms = [own] + [slots[k] for k in range(slots.shape[0])]
        while len(terms) > 1:
            terms = [sum(terms[k + 1:k + 2], terms[k]) for k in range(0, len(terms), 2)]
        return terms[0]

    pending = []

    def finish_sends():
        while pending:
            pending.pop().wait()

    def row_start(k, rowform):
        rsend[k] = rowform
        return exchange(rsend.at[k], rrecv0.at[k], rsem_s0.at[k], rsem_r0.at[k],
                        2 if direct else 0)

    def row_end(k, rowform, arrival):
        rowform = gather_sum(arrival, rowform, rrecv0.at[k])
        if not direct:
            mid[k] = rowform
            arrival = exchange(mid.at[k], rrecv1.at[k], rsem_s1.at[k], rsem_r1.at[k], 1)
            rowform = gather_sum(arrival, rowform, rrecv1.at[k])
        return rowform * (1.0 / cells)

    lane3 = lax.broadcasted_iota(jnp.int32, (by, bz), 1)
    row3 = lax.broadcasted_iota(jnp.int32, (by, bz), 0)

    def stencil(v, x_before, x_after, y_before, y_after, z_before, z_after):
        res = []
        for x in range(bx):
            here = v[x]
            xb = v[x - 1] if x > 0 else x_before
            xa = v[x + 1] if x < bx - 1 else x_after
            yb = jnp.where(row3 == 0, y_before[x], pltpu.roll(here, 1, 0))
            ya = jnp.where(row3 == by - 1, y_after[x], pltpu.roll(here, by - 1, 0))
            zb = jnp.where(lane3 == 0, z_before[x], pltpu.roll(here, 1, 1))
            za = jnp.where(lane3 == bz - 1, z_after[x], pltpu.roll(here, bz - 1, 1))
            neighbours = xa + xb + ya + yb + za + zb
            flow = (vel[0, x] * (xa - xb) + vel[1, x] * (ya - yb) + vel[2, x] * (za - zb))
            res.append((6.0 + diag[x]) * here - neighbours + 0.5 * flow)
        return res

    def dots(v, count, first=0):
        parts = []
        for i in range(ROWS):
            if first <= i < count:
                total = out[i, 0] * v[0]
                for x in range(1, bx):
                    total = total + out[i, x] * v[x]
            elif i == ROWS - 1:
                total = v[0] * v[0]
                for x in range(1, bx):
                    total = total + v[x] * v[x]
            else:
                total = None
            parts.append(jnp.zeros((1, bz), jnp.float32) if total is None
                         else jnp.sum(total, axis=0, keepdims=True))
        return jnp.sum(jnp.concatenate(parts, axis=0), axis=1, keepdims=True)

    halo_w = field_copies(0, w_ref)
    loads[0].wait()
    halo_start(halo_w)
    if direct:
        for to in partners(1):
            pl.semaphore_signal(
                ready, inc=1, device_id=to, device_id_type=pl.DeviceIdType.MESH)

    out[KEEP + 1:ROWS] = jnp.zeros((ROWS - KEEP - 1, bx, by, bz), jnp.float32)
    out[KEEP] = w_ref[...]
    loads[1].wait()
    loads[2].wait()
    wide, deep = 5, 4
    for first in range(0, KEEP, wide):
        def step(at, sums, first=first):
            sums = list(sums)
            for k in range(deep):
                i = at * deep + k
                for x in range(bx):
                    tile = kry[i, x]
                    for j in range(wide):
                        sums[j * bx + x] = sums[j * bx + x] + schur[first + j, i] * tile
            return tuple(sums)
        sums = lax.fori_loop(
            0, basis // deep, step,
            tuple(jnp.zeros((by, bz), jnp.float32) for _ in range(wide * bx)))
        for j in range(wide):
            for x in range(bx):
                out[first + j, x] = sums[j * bx + x]

    for side, (row, edge) in enumerate(((by - 1, bz - 1), (0, 0))):
        for i in range(KEEP):
            ypack[side, i] = out[i, :, row, :]
        for x in range(bx):
            packed = jnp.zeros((by, bz), jnp.float32)
            for i in range(KEEP):
                packed = jnp.where(
                    lane3 == i, pltpu.roll(out[i, x], (i - edge) % bz, 1), packed)
            zpack[side, x] = packed
    halo_r = halo_copies(
        3,
        ((out.at[0:KEEP, bx - 1], out.at[0:KEEP, 0]), (ypack.at[0], ypack.at[1]),
         (zpack.at[0], zpack.at[1])),
        tuple((r.at[0], r.at[1]) for r in (xr, yr, zr)),
    )

    row = lax.broadcasted_iota(jnp.int32, (ROWS, LANES), 0)
    lane = lax.broadcasted_iota(jnp.int32, (ROWS, LANES), 1)
    lane1 = lax.broadcasted_iota(jnp.int32, (1, LANES), 1)
    row1 = lax.broadcasted_iota(jnp.int32, (ROWS, 1), 0)

    gram = jnp.zeros((ROWS, LANES), jnp.float32)
    for j in range(KEEP + 1):
        col = dots([out[j, x] for x in range(bx)], KEEP + 1, j // 8 * 8)
        gram = jnp.where((lane == j) & (row < KEEP + 1), col, gram)
    lane8 = lax.broadcasted_iota(jnp.int32, (8, LANES), 1)
    own8 = lane8 // UNIT == lax.broadcasted_iota(jnp.int32, (8, LANES), 0)

    def spread(value):
        for shift in (UNIT, 2 * UNIT, 4 * UNIT):
            value = value + pltpu.roll(value, shift, 1)
        return value

    units = (
        gram[16:24],
        gram[8:16],
        jnp.where(lane8 < 8, gram[0:8], pltpu.roll(gram[16:24], LANES - 8, 1)),
    )
    packed = jnp.concatenate([
        jnp.sum(jnp.where(own8, spread(jnp.where(lane8 < UNIT, unit, 0.0)), 0.0),
                axis=0, keepdims=True)
        for unit in units], axis=0)
    gsend[0] = packed
    if direct:
        pl.semaphore_wait(ready, sizes[0] - 1)
    arrival0 = exchange(gsend.at[0], grecv1, gsem_s1, gsem_r1, 2 if direct else 1)

    loads[3].wait()
    loads[4].wait()
    halo_wait(halo_w)
    applied = stencil(
        [w_ref[x] for x in range(bx)], xs[0, 0], xs[0, 1],
        [ys[0, 0, x, by - 1:by, :] for x in range(bx)],
        [ys[0, 1, x, 0:1, :] for x in range(bx)],
        [zs[0, 0, x, :, bz - 1:bz] for x in range(bx)],
        [zs[0, 1, x, :, 0:1] for x in range(bx)],
    )
    for x in range(bx):
        image[0, x] = applied[x]
    ownrow = jnp.sum(jnp.where(row == lane, dots(applied, KEEP + 1), 0.0),
                     axis=0, keepdims=True)
    copies = row_start(0, ownrow)
    halo_a = field_copies(1, image.at[0])
    halo_start(halo_a)
    halo_start(halo_r)

    packed = gather_sum(arrival0, packed, grecv1)
    if not direct:
        gsend[1] = packed
        arrival1 = exchange(gsend.at[1], grecv0, gsem_s0, gsem_r0, 0)
        packed = gather_sum(arrival1, packed, grecv0)
    packed = packed * (1.0 / cells)
    units = [
        jnp.where(lane8 < UNIT,
                  spread(jnp.where(own8, jnp.broadcast_to(packed[u:u + 1], (8, LANES)), 0.0)),
                  0.0)
        for u in range(3)]
    corner = pltpu.roll(jnp.where(lane8 >= 8, units[2], 0.0), 8, 1)
    below = jnp.concatenate(
        [jnp.zeros((8, LANES), jnp.float32), jnp.where(lane8 < 8, units[1], 0.0), units[0],
         jnp.zeros((LANES - ROWS, LANES), jnp.float32)], axis=0)
    gram = jnp.concatenate(
        [jnp.where(lane8 < 8, units[2], 0.0), units[1], units[0] + corner], axis=0)
    gram = gram + below.T[0:ROWS]
    gram = jnp.where((lane < KEEP + 1) & (row < KEEP + 1), gram, 0.0)
    norm_sq = jnp.sum(
        jnp.sum(jnp.where((lane == KEEP) & (row == KEEP), gram, 0.0), axis=1, keepdims=True),
        axis=0, keepdims=True)
    scale = 1.0 / jnp.maximum(jnp.sqrt(norm_sq), 0.5)
    gram = gram * jnp.where(row == KEEP, scale, 1.0) * jnp.where(lane == KEEP, scale, 1.0)
    for x in range(bx):
        out[KEEP, x] = w_ref[x] * scale
    applied = [tile * scale for tile in applied]
    rowform = row_end(0, ownrow, copies)
    rowform = rowform * scale * jnp.where((lane1 == KEEP) | (lane1 == ROWS - 1), scale, 1.0)

    halo_wait(halo_r)
    for side in (0, 1):
        near_row, near_lane = (by - 1, bz - 1) if side == 0 else (0, 0)
        xh[side, 0] = xs[0, side] * scale
        for x in range(bx):
            yh[side, 0, x:x + 1] = ys[0, side, x, near_row:near_row + 1, :] * scale
            zh[side, x] = jnp.where(
                lane3 == KEEP, zs[0, side, x, :, near_lane:near_lane + 1] * scale, zr[side, x])
    halos = {1: halo_a}
    done = [halo_w, halo_r, halo_a]
    hcols = []
    for k in range(EXPAND):
        count = KEEP + 1 + k
        if k > 0:
            rowform = jnp.sum(jnp.where(row == lane, dots(applied, count), 0.0),
                              axis=0, keepdims=True)
            earlier = pending[:]
            pending.clear()
            arrival = row_start(k, rowform)
            for copy in earlier:
                copy.wait()
            for copies in done:
                halo_finish(copies)
            done = []
            rowform = row_end(k, rowform, arrival)
        c_row = jnp.where(lane1 < count, rowform, 0.0)
        twice = jnp.where(row == lane, 2.0, 0.0) - gram
        t_col = jnp.sum(twice * c_row, axis=1, keepdims=True)
        weights = jnp.broadcast_to(t_col, (ROWS, LANES))
        t_row = jnp.sum(jnp.where(row == lane, weights, 0.0), axis=0, keepdims=True)
        gt_row = jnp.sum(gram * weights, axis=0, keepdims=True)
        length_sq = jnp.sum(
            jnp.where(lane1 == ROWS - 1, rowform, t_row * (gt_row - 2.0 * c_row)),
            axis=1, keepdims=True)
        length_sq = jnp.maximum(length_sq, 0.0)
        length = jnp.sqrt(length_sq)
        inverse = 1.0 / jnp.maximum(length, 0.5)
        hcols.append(jnp.where(lane1 == count, length, t_row))
        newest = list(applied)
        for i in range(count):
            weight = jnp.broadcast_to(weights[i:i + 1, :], (by, bz))
            for x in range(bx):
                newest[x] = newest[x] - weight * out[i, x]
        newest = [tile * inverse for tile in newest]
        for x in range(bx):
            out[count, x] = newest[x]
        if k == EXPAND - 1:
            break
        halo_wait(halos[k + 1])
        sides = []
        for side in (0, 1):
            near_row, near_lane = (by - 1, bz - 1) if side == 0 else (0, 0)
            factor = scale if k == 0 else 1.0
            x_part = xs[k + 1, side] * factor
            y_part = [ys[k + 1, side, x, near_row:near_row + 1, :] * factor for x in range(bx)]
            y_part = jnp.concatenate(y_part, axis=0)
            for i in range(count):
                weight = weights[i:i + 1, :]
                if i < KEEP:
                    x_part = x_part - weight * xr[side, i]
                    y_part = y_part - weight * yr[side, i]
                else:
                    x_part = x_part - weight * xh[side, i - KEEP]
                    y_part = y_part - weight * yh[side, i - KEEP]
            x_part = x_part * inverse
            y_part = y_part * inverse
            z_part = []
            for x in range(bx):
                column = (zs[k + 1, side, x, :, near_lane:near_lane + 1] * factor
                          - jnp.sum(zh[side, x] * t_row, axis=1, keepdims=True)) * inverse
                z_part.append(column)
                if k + 1 < EXPAND - 1:
                    zh[side, x] = jnp.where(lane3 == count, column, zh[side, x])
            xh[side, count - KEEP] = x_part
            yh[side, count - KEEP] = y_part
            sides.append((x_part, [y_part[x:x + 1] for x in range(bx)], z_part))
        applied = stencil(newest, sides[0][0], sides[1][0], sides[0][1], sides[1][1],
                          sides[0][2], sides[1][2])
        if k + 1 < EXPAND - 1:
            for x in range(bx):
                image[1, x] = applied[x]
            halos[k + 2] = field_copies(k + 2, image.at[1])
            halo_start(halos[k + 2])
            done.append(halos[k + 2])
        e_row = t_row - c_row
        e_col = jnp.sum(jnp.where(row == lane, e_row, 0.0), axis=1, keepdims=True)
        cross_col = (e_col - jnp.sum(gram * e_row, axis=1, keepdims=True)) * inverse
        cross_row = (e_row - jnp.sum(gram * e_col, axis=0, keepdims=True)) * inverse
        corner = length_sq * inverse * inverse
        gram = jnp.where(row == count, cross_row, jnp.where(lane == count, cross_col, gram))
        gram = jnp.where((row == count) & (lane == count), corner, gram)

    for k in range(EXPAND):
        hess[k:k + 1] = hcols[k % len(hcols)]
    for copies in done:
        halo_finish(copies)
    finish_sends()


def per_device(krylov_basis, schur_vectors, next_vector, diag_shift, velocity):
    sizes = tuple(lax.axis_size(a) for a in AXES)
    block = next_vector.shape
    bx, by, bz = block
    cells = float(bx * by * bz * sizes[0] * sizes[1] * sizes[2])
    n0, n1 = sizes[1] * sizes[2], sizes[0]
    nrow = n0 * n1 if n0 * n1 <= DIRECT else n0
    nline = n0 * n1 if n0 * n1 <= DIRECT else n1
    f32 = jnp.float32
    vmem = pl.BlockSpec(memory_space=pltpu.VMEM)
    dma = pltpu.SemaphoreType.DMA
    vectors, columns = pl.pallas_call(
        functools.partial(body, sizes, cells),
        out_shape=(
            pltpu.VMEM((ROWS,) + block, f32),
            pltpu.VMEM((8, LANES), f32),
        ),
        in_specs=[
            pl.BlockSpec(memory_space=pl.ANY) for _ in range(5)
        ],
        out_specs=(vmem, vmem),
        scratch_shapes=[
            pltpu.SMEM(schur_vectors.shape[::-1], f32),
            pltpu.VMEM(block, f32),
            pltpu.VMEM(block, f32),
            pltpu.VMEM((3,) + block, f32),
            pltpu.VMEM(krylov_basis.shape, f32),
            pltpu.VMEM((2,) + block, f32),
            pltpu.VMEM((2, KEEP, by, bz), f32),
            pltpu.VMEM((2, KEEP, bx, bz), f32),
            pltpu.VMEM((2,) + block, f32),
            pltpu.VMEM((2, KEEP, bx, bz), f32),
            pltpu.VMEM((2,) + block, f32),
            pltpu.VMEM((2, EXPAND, by, bz), f32),
            pltpu.VMEM((2, EXPAND, bx, bz), f32),
            pltpu.VMEM((2,) + block, f32),
            pltpu.VMEM((EXPAND, 2, by, bz), f32),
            pltpu.VMEM((EXPAND, 2) + block, f32),
            pltpu.VMEM((EXPAND, 2) + block, f32),
            pltpu.VMEM((2, 3, LANES), f32),
            pltpu.VMEM((n0 - 1, 3, LANES), f32),
            pltpu.VMEM((nline - 1, 3, LANES), f32),
            pltpu.VMEM((EXPAND, 1, LANES), f32),
            pltpu.VMEM((EXPAND, nrow - 1, 1, LANES), f32),
            pltpu.VMEM((EXPAND, n1 - 1, 1, LANES), f32),
            pltpu.VMEM((EXPAND, 1, LANES), f32),
            dma((5,)), dma((24,)), dma((24,)),
            dma, dma, dma, dma,
            dma((EXPAND,)), dma((EXPAND,)), dma((EXPAND,)), dma((EXPAND,)),
            pltpu.SemaphoreType.REGULAR,
        ],
        compiler_params=pltpu.CompilerParams(collective_id=0, has_side_effects=True),
    )(krylov_basis, schur_vectors.T, next_vector, diag_shift, velocity)
    return vectors, columns[0:EXPAND, 0:ROWS].T


def solution(mesh):
    in_specs = (
        P(None, "gx", "gy", "gz"),
        P(),
        P("gx", "gy", "gz"),
        P("gx", "gy", "gz"),
        P(None, "gx", "gy", "gz"),
    )
    out_specs = (P(None, "gx", "gy", "gz"), P())
    return jax.shard_map(
        per_device, mesh=mesh, in_specs=in_specs, out_specs=out_specs, check_vma=False
    )
```

```python
import functools

import jax
import jax.numpy as jnp
from jax import lax
from jax.experimental import pallas as pl
from jax.experimental.pallas import tpu as pltpu
from jax.sharding import PartitionSpec as P

KEEP = 20
EXPAND = 3
ROWS = 24
LANES = 128
UNIT = 16
DIRECT = 64
AXES = ("gx", "gy", "gz")


def partner_steps(phase, sizes):
    xs = range(1, sizes[0]) if phase else ()
    steps = [(dx, 0, 0) for dx in xs] if phase == 1 else [
        (dx, dy, dz) for dx in tuple(reversed(xs)) + (0,)
        for dy in range(sizes[1]) for dz in range(sizes[2])]
    return [step for step in steps if step != (0, 0, 0)]


def body(
    sizes, cells,
    kry_hbm, schur_hbm, w_hbm, diag_hbm, vel_hbm,
    out, hess,
    schur, w_ref, diag, vel, kry, image, xr, yr, zr, ypack, zpack, xh, yh, zh, xs, ys, zs,
    gsend, grecv0, grecv1, rsend, rrecv0, rrecv1, mid,
    load_sem, halo_send, halo_recv, gsem_s0, gsem_r0, gsem_s1, gsem_r1,
    rsem_s0, rsem_r0, rsem_s1, rsem_r1, ready,
):
    place = tuple(lax.axis_index(a) for a in AXES)
    basis = kry.shape[0]
    bx, by, bz = w_ref.shape
    loads = [
        pltpu.make_async_copy(source, target, load_sem.at[k])
        for k, (source, target) in enumerate((
            (w_hbm, w_ref), (schur_hbm, schur), (kry_hbm, kry), (diag_hbm, diag), (vel_hbm, vel)))
    ]
    for copy in loads:
        copy.start()
    direct = sizes[0] * sizes[1] * sizes[2] <= DIRECT
    shifted = [[lax.rem(place[d] + k, sizes[d]) for k in range(sizes[d])] for d in range(3)]

    def partners(phase):
        return [tuple(shifted[d][step[d]] for d in range(3))
                for step in partner_steps(phase, sizes)]


    for ref in (xr, yr, zr, xs, ys, zs):
        ref[...] = jnp.zeros_like(ref)

    barrier = pltpu.get_barrier_semaphore()
    for to in partners(0) + partners(1):
        pl.semaphore_signal(
            barrier, inc=1, device_id=to, device_id_type=pl.DeviceIdType.MESH)
    pl.semaphore_wait(barrier, len(partners(0)) + len(partners(1)))

    def halo_copies(kind, sources, targets):
        found = []
        for d in range(3):
            for side in (0, 1):
                at = (kind * 3 + d) * 2 + side
                to = list(place)
                to[d] = place[d] + (1 if side == 0 else -1)
                can_send = place[d] < sizes[d] - 1 if side == 0 else place[d] > 0
                can_recv = place[d] > 0 if side == 0 else place[d] < sizes[d] - 1
                found.append((
                    pltpu.make_async_remote_copy(
                        src_ref=sources[d][side], dst_ref=targets[d][side],
                        send_sem=halo_send.at[at], recv_sem=halo_recv.at[at],
                        device_id=tuple(to), device_id_type=pl.DeviceIdType.MESH,
                    ), can_send, can_recv))
        return found

    def halo_start(copies):
        for copy, can_send, _ in copies:
            pl.when(can_send)(copy.start)

    def halo_wait(copies):
        for copy, _, can_recv in copies:
            pl.when(can_recv)(copy.wait_recv)

    def halo_finish(copies):
        for copy, can_send, _ in copies:
            pl.when(can_send)(copy.wait_send)

    def field_copies(kind, ref):
        return halo_copies(
            kind,
            ((ref.at[bx - 1], ref.at[0]), (ref, ref), (ref, ref)),
            tuple((r.at[kind, 0], r.at[kind, 1]) for r in (xs, ys, zs)),
        )

    def exchange(send, slots, sem_s, sem_r, phase):
        for at, to in enumerate(partners(phase)):
            pltpu.make_async_remote_copy(
                src_ref=send, dst_ref=slots.at[at], send_sem=sem_s, recv_sem=sem_r,
                device_id=to, device_id_type=pl.DeviceIdType.MESH,
            ).start()
        pending.append(pltpu.make_async_copy(slots, slots, sem_s))
        return pltpu.make_async_copy(slots, slots, sem_r)

    def gather_sum(arrival, own, slots):
        arrival.wait()
        terms = [own] + [slots[k] for k in range(slots.shape[0])]
        while len(terms) > 1:
            terms = [sum(terms[k + 1:k + 2], terms[k]) for k in range(0, len(terms), 2)]
        return terms[0]

    pending = []

    def finish_sends():
        while pending:
            pending.pop().wait()

    def row_start(k, rowform):
        rsend[k] = rowform
        return exchange(rsend.at[k], rrecv0.at[k], rsem_s0.at[k], rsem_r0.at[k],
                        2 if direct else 0)

    def row_end(k, rowform, arrival):
        rowform = gather_sum(arrival, rowform, rrecv0.at[k])
        if not direct:
            mid[k] = rowform
            arrival = exchange(mid.at[k], rrecv1.at[k], rsem_s1.at[k], rsem_r1.at[k], 1)
            rowform = gather_sum(arrival, rowform, rrecv1.at[k])
        return rowform * (1.0 / cells)

    lane3 = lax.broadcasted_iota(jnp.int32, (by, bz), 1)
    row3 = lax.broadcasted_iota(jnp.int32, (by, bz), 0)

    def stencil(v, x_before, x_after, y_before, y_after, z_before, z_after):
        res = []
        for x in range(bx):
            here = v[x]
            xb = v[x - 1] if x > 0 else x_before
            xa = v[x + 1] if x < bx - 1 else x_after
            yb = jnp.where(row3 == 0, y_before[x], pltpu.roll(here, 1, 0))
            ya = jnp.where(row3 == by - 1, y_after[x], pltpu.roll(here, by - 1, 0))
            zb = jnp.where(lane3 == 0, z_before[x], pltpu.roll(here, 1, 1))
            za = jnp.where(lane3 == bz - 1, z_after[x], pltpu.roll(here, bz - 1, 1))
            neighbours = xa + xb + ya + yb + za + zb
            flow = (vel[0, x] * (xa - xb) + vel[1, x] * (ya - yb) + vel[2, x] * (za - zb))
            res.append((6.0 + diag[x]) * here - neighbours + 0.5 * flow)
        return res

    def dots(v, count, first=0):
        parts = []
        for i in range(ROWS):
            if first <= i < count:
                total = out[i, 0] * v[0]
                for x in range(1, bx):
                    total = total + out[i, x] * v[x]
            elif i == ROWS - 1:
                total = v[0] * v[0]
                for x in range(1, bx):
                    total = total + v[x] * v[x]
            else:
                total = None
            parts.append(jnp.zeros((1, bz), jnp.float32) if total is None
                         else jnp.sum(total, axis=0, keepdims=True))
        return jnp.sum(jnp.concatenate(parts, axis=0), axis=1, keepdims=True)

    halo_w = field_copies(0, w_ref)
    loads[0].wait()
    halo_start(halo_w)
    if direct:
        for to in partners(1):
            pl.semaphore_signal(
                ready, inc=1, device_id=to, device_id_type=pl.DeviceIdType.MESH)

    out[KEEP + 1:ROWS] = jnp.zeros((ROWS - KEEP - 1, bx, by, bz), jnp.float32)
    out[KEEP] = w_ref[...]
    loads[1].wait()
    loads[2].wait()
    wide, deep = 5, 4
    for first in range(0, KEEP, wide):
        def step(at, sums, first=first):
            sums = list(sums)
            for k in range(deep):
                i = at * deep + k
                for x in range(bx):
                    tile = kry[i, x]
                    for j in range(wide):
                        sums[j * bx + x] = sums[j * bx + x] + schur[first + j, i] * tile
            return tuple(sums)
        sums = lax.fori_loop(
            0, basis // deep, step,
            tuple(jnp.zeros((by, bz), jnp.float32) for _ in range(wide * bx)))
        for j in range(wide):
            for x in range(bx):
                out[first + j, x] = sums[j * bx + x]

    row = lax.broadcasted_iota(jnp.int32, (ROWS, LANES), 0)
    lane = lax.broadcasted_iota(jnp.int32, (ROWS, LANES), 1)
    lane1 = lax.broadcasted_iota(jnp.int32, (1, LANES), 1)
    row1 = lax.broadcasted_iota(jnp.int32, (ROWS, 1), 0)

    gram = jnp.zeros((ROWS, LANES), jnp.float32)
    for j in range(KEEP + 1):
        col = dots([out[j, x] for x in range(bx)], KEEP + 1, j // 8 * 8)
        gram = jnp.where((lane == j) & (row < KEEP + 1), col, gram)
    lane8 = lax.broadcasted_iota(jnp.int32, (8, LANES), 1)
    own8 = lane8 // UNIT == lax.broadcasted_iota(jnp.int32, (8, LANES), 0)

    def spread(value):
        for shift in (UNIT, 2 * UNIT, 4 * UNIT):
            value = value + pltpu.roll(value, shift, 1)
        return value

    units = (
        gram[16:24],
        gram[8:16],
        jnp.where(lane8 < 8, gram[0:8], pltpu.roll(gram[16:24], LANES - 8, 1)),
    )
    packed = jnp.concatenate([
        jnp.sum(jnp.where(own8, spread(jnp.where(lane8 < UNIT, unit, 0.0)), 0.0),
                axis=0, keepdims=True)
        for unit in units], axis=0)
    gsend[0] = packed
    if direct:
        pl.semaphore_wait(ready, sizes[0] - 1)
    arrival0 = exchange(gsend.at[0], grecv1, gsem_s1, gsem_r1, 2 if direct else 1)

    loads[3].wait()
    loads[4].wait()
    halo_wait(halo_w)
    applied = stencil(
        [w_ref[x] for x in range(bx)], xs[0, 0], xs[0, 1],
        [ys[0, 0, x, by - 1:by, :] for x in range(bx)],
        [ys[0, 1, x, 0:1, :] for x in range(bx)],
        [zs[0, 0, x, :, bz - 1:bz] for x in range(bx)],
        [zs[0, 1, x, :, 0:1] for x in range(bx)],
    )
    for x in range(bx):
        image[0, x] = applied[x]
    ownrow = jnp.sum(jnp.where(row == lane, dots(applied, KEEP + 1), 0.0),
                     axis=0, keepdims=True)
    copies = row_start(0, ownrow)
    halo_a = field_copies(1, image.at[0])
    halo_start(halo_a)

    for side, (near, edge) in enumerate(((by - 1, bz - 1), (0, 0))):
        for i in range(KEEP):
            ypack[side, i] = out[i, :, near, :]
        for x in range(bx):
            face = jnp.zeros((by, bz), jnp.float32)
            for i in range(KEEP):
                face = jnp.where(
                    lane3 == i, pltpu.roll(out[i, x], (i - edge) % bz, 1), face)
            zpack[side, x] = face
    halo_r = halo_copies(
        3,
        ((out.at[0:KEEP, bx - 1], out.at[0:KEEP, 0]), (ypack.at[0], ypack.at[1]),
         (zpack.at[0], zpack.at[1])),
        tuple((r.at[0], r.at[1]) for r in (xr, yr, zr)),
    )
    halo_start(halo_r)

    packed = gather_sum(arrival0, packed, grecv1)
    if not direct:
        gsend[1] = packed
        arrival1 = exchange(gsend.at[1], grecv0, gsem_s0, gsem_r0, 0)
        packed = gather_sum(arrival1, packed, grecv0)
    packed = packed * (1.0 / cells)
    units = [
        jnp.where(lane8 < UNIT,
                  spread(jnp.where(own8, jnp.broadcast_to(packed[u:u + 1], (8, LANES)), 0.0)),
                  0.0)
        for u in range(3)]
    corner = pltpu.roll(jnp.where(lane8 >= 8, units[2], 0.0), 8, 1)
    below = jnp.concatenate(
        [jnp.zeros((8, LANES), jnp.float32), jnp.where(lane8 < 8, units[1], 0.0), units[0],
         jnp.zeros((LANES - ROWS, LANES), jnp.float32)], axis=0)
    gram = jnp.concatenate(
        [jnp.where(lane8 < 8, units[2], 0.0), units[1], units[0] + corner], axis=0)
    gram = gram + below.T[0:ROWS]
    gram = jnp.where((lane < KEEP + 1) & (row < KEEP + 1), gram, 0.0)
    norm_sq = jnp.sum(
        jnp.sum(jnp.where((lane == KEEP) & (row == KEEP), gram, 0.0), axis=1, keepdims=True),
        axis=0, keepdims=True)
    scale = 1.0 / jnp.maximum(jnp.sqrt(norm_sq), 0.5)
    gram = gram * jnp.where(row == KEEP, scale, 1.0) * jnp.where(lane == KEEP, scale, 1.0)
    for x in range(bx):
        out[KEEP, x] = w_ref[x] * scale
    applied = [tile * scale for tile in applied]
    rowform = row_end(0, ownrow, copies)
    rowform = rowform * scale * jnp.where((lane1 == KEEP) | (lane1 == ROWS - 1), scale, 1.0)

    halo_wait(halo_r)
    for side in (0, 1):
        near_row, near_lane = (by - 1, bz - 1) if side == 0 else (0, 0)
        xh[side, 0] = xs[0, side] * scale
        for x in range(bx):
            yh[side, 0, x:x + 1] = ys[0, side, x, near_row:near_row + 1, :] * scale
            zh[side, x] = jnp.where(
                lane3 == KEEP, zs[0, side, x, :, near_lane:near_lane + 1] * scale, zr[side, x])
    halos = {1: halo_a}
    done = [halo_w, halo_r, halo_a]
    hcols = []
    for k in range(EXPAND):
        count = KEEP + 1 + k
        if k > 0:
            rowform = jnp.sum(jnp.where(row == lane, dots(applied, count), 0.0),
                              axis=0, keepdims=True)
            earlier = pending[:]
            pending.clear()
            arrival = row_start(k, rowform)
            for copy in earlier:
                copy.wait()
            for copies in done:
                halo_finish(copies)
            done = []
            rowform = row_end(k, rowform, arrival)
        c_row = jnp.where(lane1 < count, rowform, 0.0)
        twice = jnp.where(row == lane, 2.0, 0.0) - gram
        t_col = jnp.sum(twice * c_row, axis=1, keepdims=True)
        weights = jnp.broadcast_to(t_col, (ROWS, LANES))
        t_row = jnp.sum(jnp.where(row == lane, weights, 0.0), axis=0, keepdims=True)
        gt_row = jnp.sum(gram * weights, axis=0, keepdims=True)
        length_sq = jnp.sum(
            jnp.where(lane1 == ROWS - 1, rowform, t_row * (gt_row - 2.0 * c_row)),
            axis=1, keepdims=True)
        length_sq = jnp.maximum(length_sq, 0.0)
        length = jnp.sqrt(length_sq)
        inverse = 1.0 / jnp.maximum(length, 0.5)
        hcols.append(jnp.where(lane1 == count, length, t_row))
        newest = list(applied)
        for i in range(count):
            weight = jnp.broadcast_to(weights[i:i + 1, :], (by, bz))
            for x in range(bx):
                newest[x] = newest[x] - weight * out[i, x]
        newest = [tile * inverse for tile in newest]
        for x in range(bx):
            out[count, x] = newest[x]
        if k == EXPAND - 1:
            break
        halo_wait(halos[k + 1])
        sides = []
        for side in (0, 1):
            near_row, near_lane = (by - 1, bz - 1) if side == 0 else (0, 0)
            factor = scale if k == 0 else 1.0
            x_part = xs[k + 1, side] * factor
            y_part = [ys[k + 1, side, x, near_row:near_row + 1, :] * factor for x in range(bx)]
            y_part = jnp.concatenate(y_part, axis=0)
            for i in range(count):
                weight = weights[i:i + 1, :]
                if i < KEEP:
                    x_part = x_part - weight * xr[side, i]
                    y_part = y_part - weight * yr[side, i]
                else:
                    x_part = x_part - weight * xh[side, i - KEEP]
                    y_part = y_part - weight * yh[side, i - KEEP]
            x_part = x_part * inverse
            y_part = y_part * inverse
            z_part = []
            for x in range(bx):
                column = (zs[k + 1, side, x, :, near_lane:near_lane + 1] * factor
                          - jnp.sum(zh[side, x] * t_row, axis=1, keepdims=True)) * inverse
                z_part.append(column)
                if k + 1 < EXPAND - 1:
                    zh[side, x] = jnp.where(lane3 == count, column, zh[side, x])
            xh[side, count - KEEP] = x_part
            yh[side, count - KEEP] = y_part
            sides.append((x_part, [y_part[x:x + 1] for x in range(bx)], z_part))
        applied = stencil(newest, sides[0][0], sides[1][0], sides[0][1], sides[1][1],
                          sides[0][2], sides[1][2])
        if k + 1 < EXPAND - 1:
            for x in range(bx):
                image[1, x] = applied[x]
            halos[k + 2] = field_copies(k + 2, image.at[1])
            halo_start(halos[k + 2])
            done.append(halos[k + 2])
        e_row = t_row - c_row
        e_col = jnp.sum(jnp.where(row == lane, e_row, 0.0), axis=1, keepdims=True)
        cross_col = (e_col - jnp.sum(gram * e_row, axis=1, keepdims=True)) * inverse
        cross_row = (e_row - jnp.sum(gram * e_col, axis=0, keepdims=True)) * inverse
        corner = length_sq * inverse * inverse
        gram = jnp.where(row == count, cross_row, jnp.where(lane == count, cross_col, gram))
        gram = jnp.where((row == count) & (lane == count), corner, gram)

    for k in range(EXPAND):
        hess[k:k + 1] = hcols[k % len(hcols)]
    for copies in done:
        halo_finish(copies)
    finish_sends()


def per_device(krylov_basis, schur_vectors, next_vector, diag_shift, velocity):
    sizes = tuple(lax.axis_size(a) for a in AXES)
    block = next_vector.shape
    bx, by, bz = block
    cells = float(bx * by * bz * sizes[0] * sizes[1] * sizes[2])
    n0, n1 = sizes[1] * sizes[2], sizes[0]
    nrow = n0 * n1 if n0 * n1 <= DIRECT else n0
    nline = n0 * n1 if n0 * n1 <= DIRECT else n1
    f32 = jnp.float32
    vmem = pl.BlockSpec(memory_space=pltpu.VMEM)
    dma = pltpu.SemaphoreType.DMA
    vectors, columns = pl.pallas_call(
        functools.partial(body, sizes, cells),
        out_shape=(
            pltpu.VMEM((ROWS,) + block, f32),
            pltpu.VMEM((8, LANES), f32),
        ),
        in_specs=[
            pl.BlockSpec(memory_space=pl.ANY) for _ in range(5)
        ],
        out_specs=(vmem, vmem),
        scratch_shapes=[
            pltpu.SMEM(schur_vectors.shape[::-1], f32),
            pltpu.VMEM(block, f32),
            pltpu.VMEM(block, f32),
            pltpu.VMEM((3,) + block, f32),
            pltpu.VMEM(krylov_basis.shape, f32),
            pltpu.VMEM((2,) + block, f32),
            pltpu.VMEM((2, KEEP, by, bz), f32),
            pltpu.VMEM((2, KEEP, bx, bz), f32),
            pltpu.VMEM((2,) + block, f32),
            pltpu.VMEM((2, KEEP, bx, bz), f32),
            pltpu.VMEM((2,) + block, f32),
            pltpu.VMEM((2, EXPAND, by, bz), f32),
            pltpu.VMEM((2, EXPAND, bx, bz), f32),
            pltpu.VMEM((2,) + block, f32),
            pltpu.VMEM((EXPAND, 2, by, bz), f32),
            pltpu.VMEM((EXPAND, 2) + block, f32),
            pltpu.VMEM((EXPAND, 2) + block, f32),
            pltpu.VMEM((2, 3, LANES), f32),
            pltpu.VMEM((n0 - 1, 3, LANES), f32),
            pltpu.VMEM((nline - 1, 3, LANES), f32),
            pltpu.VMEM((EXPAND, 1, LANES), f32),
            pltpu.VMEM((EXPAND, nrow - 1, 1, LANES), f32),
            pltpu.VMEM((EXPAND, n1 - 1, 1, LANES), f32),
            pltpu.VMEM((EXPAND, 1, LANES), f32),
            dma((5,)), dma((24,)), dma((24,)),
            dma, dma, dma, dma,
            dma((EXPAND,)), dma((EXPAND,)), dma((EXPAND,)), dma((EXPAND,)),
            pltpu.SemaphoreType.REGULAR,
        ],
        compiler_params=pltpu.CompilerParams(collective_id=0, has_side_effects=True),
    )(krylov_basis, schur_vectors.T, next_vector, diag_shift, velocity)
    return vectors, columns[0:EXPAND, 0:ROWS].T


def solution(mesh):
    in_specs = (
        P(None, "gx", "gy", "gz"),
        P(),
        P("gx", "gy", "gz"),
        P("gx", "gy", "gz"),
        P(None, "gx", "gy", "gz"),
    )
    out_specs = (P(None, "gx", "gy", "gz"), P())
    return jax.shard_map(
        per_device, mesh=mesh, in_specs=in_specs, out_specs=out_specs, check_vma=False
    )
```
